512 devices in a mesh: wide: 128 (over x, z, core), narrow: 4 (over y).
Axes of the slice: x: 4, y: 4, z: 16, core: 2. Of those that a mesh axis runs over, the one named last changes fastest.
Arguments:
- queries: bfloat16 [65536, 2048], P(('wide', 'narrow')), may hold values from -12 to 12
- keys: bfloat16 [65536, 2048], P(('wide', 'narrow')), may hold values from -24 to 24
- values: bfloat16 [65536, 2048], P(('wide', 'narrow')), may hold values from -6 to 6
- view_lengths: int32 [128, 4], P('wide'), may hold values from 1 to 256, 512 in all within a row
- gain: float32 [2048], replicated, may hold values from 0.25 to 1.75
- w_gate: bfloat16 [4, 512, 512], P('narrow', 'wide'), may hold values from -0.25 to 0.25
- w_up: bfloat16 [4, 512, 512], P('narrow', 'wide'), may hold values from -0.25 to 0.25
- w_down: bfloat16 [4, 512, 512], P('narrow', 'wide'), may hold values from -0.25 to 0.25
- m_gate: float32 [4, 512, 512], P('narrow', 'wide'), may hold values from -4 to 4
- m_up: float32 [4, 512, 512], P('narrow', 'wide'), may hold values from -4 to 4
- m_down: float32 [4, 512, 512], P('narrow', 'wide'), may hold values from -4 to 4
Outputs:
- output: bfloat16 [65536, 2048], P(('wide', 'narrow'))
- new_gate: bfloat16 [4, 512, 512], P('narrow', 'wide')
- new_up: bfloat16 [4, 512, 512], P('narrow', 'wide')
- new_down: bfloat16 [4, 512, 512], P('narrow', 'wide')
- mom_gate: float32 [4, 512, 512], P('narrow', 'wide')
- mom_up: float32 [4, 512, 512], P('narrow', 'wide')
- mom_down: float32 [4, 512, 512], P('narrow', 'wide')
The draws below stay inside these ranges and needn't reach their ends.
Inputs may be any that keep to these rules, and one draw needn't show every extreme that they name: `view_lengths`: each row sums to 512; its largest entry is 256.
All inputs are finite; a program needn't handle non-finite values.
Results may differ from the reference program's by a relative error of at most 0.0091.
Values may be sent and summed in bfloat16 or wider, within the bound.
A program may use at most 64 MiB of HBM per device.

```python
import math
import jax
import jax.numpy as jnp
import numpy as np
from jax import lax

HEAD = 512
HEADS = 4
VIEWS = 4
D = 2048
GROUP = 512
GROUPS = 128
TOKENS = 65536


def lifted_directions(key):
    base = jax.random.fold_in(key, 7001)
    flips = jax.random.bernoulli(jax.random.fold_in(base, 1), 0.5, (GROUPS, HEADS, HEAD))
    signs = jnp.where(flips, 1.0, -1.0).astype(jnp.float32)
    orders = [jax.random.permutation(jax.random.fold_in(base, 10 + number), GROUPS) for number in range(HEADS)]
    ranking = jnp.stack(orders, axis=1).astype(jnp.float32)
    chosen = max(2, GROUPS // 4)
    strength = jnp.maximum(320.0 - 210.0 * ranking / (chosen - 1), 0.0)
    amplitude = jnp.where(ranking < chosen, jnp.sqrt(strength / math.sqrt(HEAD)), 0.0)
    return signs * amplitude[:, :, None]


def noise_field(key, shape):
    return jax.random.truncated_normal(key, -6.0, 6.0, shape, jnp.float32)


def draw_queries(key, part):
    lifted = lifted_directions(key)
    noise = noise_field(jax.random.fold_in(key, 11), (GROUPS, GROUP, HEADS, HEAD))
    field = noise + lifted[:, None]
    return field.reshape(TOKENS, D).astype(jnp.bfloat16)


def draw_keys(key, part):
    lifted = lifted_directions(key)
    noise = noise_field(jax.random.fold_in(key, 12), (GROUPS, GROUP, HEADS, GROUPS, HEAD // GROUPS))
    pairing = jax.random.permutation(jax.random.fold_in(key, 13), GROUPS)
    boost = jnp.where(pairing[:, None] == jnp.arange(GROUPS)[None, :], 3.0, 1.0).astype(jnp.float32)
    field = noise * boost[:, None, None, :, None] + lifted.reshape(GROUPS, 1, HEADS, GROUPS, HEAD // GROUPS)
    return field.reshape(TOKENS, D).astype(jnp.bfloat16)


def level_of(stream_key, extent, shards, smallest, largest):
    factor_of = 1.0
    for dim, parts in shards:
        steps = jax.random.uniform(jax.random.fold_in(jax.random.fold_in(stream_key, 6), dim), (parts,), jnp.float32, smallest / len(shards), largest / len(shards))
        factor_of = factor_of * jnp.repeat(jnp.exp(steps), extent[dim] // parts).reshape((-1,) + (1,) * (len(extent) - 1 - dim))
    return factor_of


def profile(number_of, total, limit, skew):
    loads = [(1 << 20) // math.isqrt(rank ** skew) + 1 for rank in range(2, number_of + 1)]
    rest, counts = total - limit - (number_of - 1), [1] * (number_of - 1)
    while rest > 0:
        candidates = [i for i in range(number_of - 1) if counts[i] < limit]
        mass, budget = sum([loads[i] for i in candidates]), rest
        for i in candidates:
            more = min(limit - counts[i], max(1, budget * loads[i] // mass), rest)
            counts[i] = counts[i] + more
            rest = rest - more
    return np.array([limit] + counts)


def uneven_parts(stream_key, amount, total, most, slope):
    if amount == 2:
        one = jax.random.randint(stream_key, (), max(1, total - most), min(most, total - 1) + 1)
        return jnp.stack([one, total - one])
    sizes = jnp.asarray(profile(amount, total, most, slope), jnp.int32)
    couples = (amount - 1) // 2
    source_of, taker = sizes[1:1 + 2 * couples:2], sizes[2:2 + 2 * couples:2]
    margin = jnp.minimum(source_of - 1, most - taker)
    passed = jax.random.randint(jax.random.fold_in(stream_key, 1), (couples,), 0, 1 << 20) % (margin + 1)
    sizes = sizes.at[1:1 + 2 * couples:2].set(source_of - passed).at[2:2 + 2 * couples:2].set(taker + passed)
    return sizes[jax.random.permutation(jax.random.fold_in(stream_key, 2), amount)]


def normal_values(rng, shape, scale, limit, split=(), kind=jnp.bfloat16):
    entries = jax.random.normal(rng, shape, jnp.float32) * scale
    if len(split) > 0:
        entries = level_of(rng, shape, split, -0.22, 0.18) * entries
    return jnp.clip(entries, min=-limit, max=limit).astype(kind)


def setup_inputs(seed: int = 0) -> dict:
    key_of = jax.random.split(jax.random.key(seed), 12)
    return {
        "queries": draw_queries(jax.random.fold_in(key_of[11], 71), 0),
        "keys": draw_keys(jax.random.fold_in(key_of[11], 71), 0),
        "values": normal_values(key_of[2], (TOKENS, D), 1.0, 6.0, ((0, 512),)),
        "view_lengths": jax.vmap(lambda own: uneven_parts(own, VIEWS, GROUP, GROUP // 2, 1))(jax.random.split(key_of[3], GROUPS)).reshape((GROUPS, VIEWS)).astype(jnp.int32),
        "gain": jnp.clip(1.0 + 0.15 * jax.random.normal(key_of[4], (D,), jnp.float32), 0.25, 1.75),
        "w_gate": normal_values(key_of[5], (HEADS, HEAD, HEAD), HEAD ** -0.5, 0.25, ((0, 4), (1, 128))),
        "w_up": normal_values(key_of[6], (HEADS, HEAD, HEAD), HEAD ** -0.5, 0.25, ((0, 4), (1, 128))),
        "w_down": normal_values(key_of[7], (HEADS, HEAD, HEAD), HEAD ** -0.5, 0.25, ((0, 4), (1, 128))),
        "m_gate": normal_values(key_of[8], (HEADS, HEAD, HEAD), 0.5, 4.0, ((0, 4), (1, 128)), jnp.float32),
        "m_up": normal_values(key_of[9], (HEADS, HEAD, HEAD), 0.5, 4.0, ((0, 4), (1, 128)), jnp.float32),
        "m_down": normal_values(key_of[10], (HEADS, HEAD, HEAD), 0.5, 4.0, ((0, 4), (1, 128)), jnp.float32),
    }


momentum_decay = 0.9
step_size = 0.02
epsilon = 1e-06
highest_precision = lax.Precision.HIGHEST

def attend(query_rows, key_rows, value_rows, query_ids, key_ids):
    scaling = query_rows.shape[-1] ** (-0.5)
    scores = jnp.einsum('rhd,ghd->hrg', query_rows.astype(jnp.float32), key_rows.astype(jnp.float32), precision=highest_precision) * scaling
    allowed = query_ids[:, None] == key_ids[None, :]
    scores = jnp.where(allowed[None], scores, -1e+30)
    highest = lax.optimization_barrier(jnp.max(scores, axis=-1, keepdims=True))
    expo = jnp.exp(scores - highest)
    probs = (expo / lax.optimization_barrier(jnp.sum(expo, axis=-1, keepdims=True))).astype(jnp.bfloat16)
    return jnp.einsum('hrg,ghd->rhd', probs.astype(jnp.float32), value_rows.astype(jnp.float32), precision=highest_precision)

def rms_gain(field, gains):
    return field * lax.rsqrt(lax.optimization_barrier(jnp.mean(field * field, axis=-1, keepdims=True)) + epsilon) * gains

def silu_slope(pre):
    sig = jax.nn.sigmoid(pre)
    return sig * (1.0 + pre * (1.0 - sig))

def wide_dot(left, right, dims):
    return lax.dot_general(left.astype(jnp.float32), right.astype(jnp.float32), dims, precision=highest_precision, preferred_element_type=jnp.float32)

def gradients(key_rows, value_rows, gate_full, up_full, down_full):
    plain = (((1,), (0,)), ((), ()))
    pre_gate = wide_dot(key_rows, gate_full, plain)
    pre_up = wide_dot(key_rows, up_full, plain)
    activ = jax.nn.silu(pre_gate)
    hidden = (activ * pre_up).astype(jnp.bfloat16)
    d_hidden = -wide_dot(value_rows, down_full, (((1,), (1,)), ((), ())))
    d_gate = (d_hidden * pre_up * silu_slope(pre_gate)).astype(jnp.bfloat16)
    d_up = (d_hidden * activ).astype(jnp.bfloat16)
    contract = (((0,), (0,)), ((), ()))
    grad_gate = wide_dot(key_rows, d_gate, contract)
    grad_up = wide_dot(key_rows, d_up, contract)
    grad_down = -wide_dot(hidden, value_rows, contract)
    return (grad_gate, grad_up, grad_down)

def renormed(weight, moment, radius):
    old = weight.astype(jnp.float32)
    moved = old - step_size * moment / radius
    ratio = jnp.sqrt(lax.optimization_barrier(jnp.sum(old * old, axis=-1, keepdims=True)) + epsilon) / jnp.sqrt(lax.optimization_barrier(jnp.sum(moved * moved, axis=-1, keepdims=True)) + epsilon)
    return (moved * ratio).astype(jnp.bfloat16)

def apply_fast(query_rows, gate_full, up_full, down_full, gains):
    plain = (((1,), (0,)), ((), ()))
    pre_gate = wide_dot(query_rows, gate_full, plain)
    pre_up = wide_dot(query_rows, up_full, plain)
    hidden = (jax.nn.silu(pre_gate) * pre_up).astype(jnp.bfloat16)
    fast_raw = wide_dot(hidden, down_full, plain)
    return rms_gain(fast_raw, gains).astype(jnp.bfloat16)

def view_ids_of(lengths):
    ends = jnp.cumsum(lengths.astype(jnp.int32))
    position = jnp.arange(GROUP, dtype=jnp.int32)
    return lax.optimization_barrier(jnp.sum((position[:, None] >= ends[None, :-1]).astype(jnp.int32), axis=1)).astype(jnp.int32)

def reference(queries, keys, values, view_lengths, gain, w_gate, w_up, w_down, m_gate, m_up, m_down):
    head_gains = gain.reshape(HEADS, HEAD)
    grouped_q = queries.reshape(GROUPS, GROUP, HEADS, HEAD)
    grouped_k = keys.reshape(GROUPS, GROUP, HEADS, HEAD)
    grouped_v = values.reshape(GROUPS, GROUP, HEADS, HEAD)
    head_grads = jax.vmap(gradients, in_axes=(1, 1, 0, 0, 0))

    def accumulate(totals, pair):
        terms = head_grads(pair[0], pair[1], w_gate, w_up, w_down)
        return (tuple((total + term for total, term in zip(totals, terms))), None)
    zeros = jnp.zeros((HEADS, HEAD, HEAD), jnp.float32)
    grads, unused = lax.scan(accumulate, (zeros, zeros, zeros), (grouped_k, grouped_v))
    grad_scale = TOKENS ** (-0.5)
    moments = tuple((momentum_decay * moment + grad * grad_scale for moment, grad in zip((m_gate, m_up, m_down), grads)))
    fresh = tuple((renormed(weight, moment, jnp.sqrt(lax.optimization_barrier(jnp.mean(moment * moment, axis=(1, 2), keepdims=True)) + epsilon)) for weight, moment in zip((w_gate, w_up, w_down), moments)))
    head_apply = jax.vmap(apply_fast, in_axes=(1, 0, 0, 0, 0), out_axes=1)

    def group_output(inputs):
        query_rows, key_rows, value_rows, lengths = inputs
        ids = view_ids_of(lengths)
        attn = attend(query_rows, key_rows, value_rows, ids, ids)
        view_out = rms_gain(attn, head_gains).astype(jnp.bfloat16)
        fast_out = head_apply(query_rows, fresh[0], fresh[1], fresh[2], head_gains)
        return (view_out.astype(jnp.float32) + fast_out.astype(jnp.float32)).astype(jnp.bfloat16)
    output = lax.map(group_output, (grouped_q, grouped_k, grouped_v, view_lengths)).reshape(TOKENS, D)
    return (output, fresh[0], fresh[1], fresh[2], moments[0], moments[1], moments[2])
```

```python
import functools

import jax
import jax.numpy as jnp
from jax import lax
from jax.experimental import pallas as pl
from jax.experimental.pallas import tpu as pltpu
from jax.sharding import Mesh
from jax.sharding import PartitionSpec as P

WIDE = ("wide_0", "wide_1", "wide_2")
WIDE_NARROW = ("wide_0", "wide_1", "wide_2", "narrow")
MESH = pl.DeviceIdType.MESH

momentum_decay = 0.9
step_size = 0.02
epsilon = 1e-06

NX, NZ, NY = 4, 16, 4
HEAD = 512
HALF = 256
GROUP = 512
TOK = 128
CHIPS = NX * NZ
TOKENS = 65536
F32 = jnp.float32
BF16 = jnp.bfloat16


def nt(a, b):
    return lax.dot_general(a, b, (((1,), (1,)), ((), ())), preferred_element_type=F32)


def mm(a, b):
    return jnp.dot(a, b, preferred_element_type=F32)


def rms(field, gains):
    return field * lax.rsqrt(jnp.mean(field * field, axis=-1, keepdims=True) + epsilon) * gains


def remote(src, dst, send, recv, **where):
    return pltpu.make_async_remote_copy(
        src_ref=src, dst_ref=dst, send_sem=send, recv_sem=recv, device_id=where, device_id_type=MESH
    )


def loop(n, body, start=0):
    def step(i, carry):
        body(i)
        return carry

    lax.fori_loop(start, n, step, 0)


def kernel(
    q_in, k_in, v_in, lengths, gain, wg, wu, wd, mg, mu, md,
    out, ng, nu, nd, og, ou, od,
    qh, kh, vh, kt, ht, hid, dg, du, ex, exr, mhalf, wbuf, w2, own, gsend, grecv,
    xs, xr, zs, zr, mbuf, n2, view, oblk,
    tok_send, tok_recv, tok_own, ex_sem, wz_s, wz_r, wx_s, wx_r, wc_s, wc_r,
    mz_s, mz_r, mx_s, mx_r, mc_s, mc_r, gs_s, gs_r, rx_s, rx_r, rz_s, rz_r, o_s, o_r, o_own,
):
    x = lax.axis_index("wide_0")
    z = lax.axis_index("wide_1")
    c = lax.axis_index("wide_2")
    y = lax.axis_index("narrow")
    chip = x * NZ + z
    other = 1 - c

    for t, w in enumerate((wg, wu, wd)):
        ex[t] = w[0].astype(F32)
    for t, m in enumerate((mg, mu, md)):
        ex[3 + t] = m[0]

    barrier = pltpu.get_barrier_semaphore()
    pl.semaphore_signal(barrier, inc=1, device_id={"wide_2": other}, device_id_type=MESH)
    for d in range(1, NY):
        pl.semaphore_signal(
            barrier, inc=1, device_id={"narrow": lax.rem(y + d, NY)}, device_id_type=MESH
        )
    for d in range(1, NX):
        pl.semaphore_signal(
            barrier, inc=1, device_id={"wide_0": lax.rem(x + d, NX)}, device_id_type=MESH
        )

    def greet(d):
        pl.semaphore_signal(
            barrier, inc=1, device_id={"wide_1": lax.rem(z + d, NZ)}, device_id_type=MESH
        )

    loop(NZ, greet, 1)
    pl.semaphore_wait(barrier, NY - 1 + NX - 1 + NZ - 1 + 1)

    def cols(who):
        return pl.ds(pl.multiple_of(who * HEAD, HEAD), HEAD)

    def rows(who):
        return pl.ds(pl.multiple_of(who * TOK, TOK), TOK)

    trio = ((k_in, kh), (v_in, vh), (q_in, qh))

    def tok_copy(t, d):
        src, dst = trio[t]
        to = lax.rem(y + d, NY)
        return remote(
            src.at[:, cols(to)], dst.at[rows(y)], tok_send.at[t, d], tok_recv.at[t, d], narrow=to
        )

    def tok_wait(t):
        src, dst = trio[t]
        for d in range(1, NY):
            frm = lax.rem(y + NY - d, NY)
            remote(
                src.at[:, cols(y)], dst.at[rows(frm)], tok_send.at[t, d], tok_recv.at[t, d], narrow=frm
            ).wait_recv()
        tok_local(t).wait()

    def tok_local(t):
        src, dst = trio[t]
        return pltpu.make_async_copy(src.at[:, cols(y)], dst.at[rows(y)], tok_own.at[t])

    swap = remote(ex, exr, ex_sem.at[0], ex_sem.at[1], wide_2=other)
    swap.start()
    for t in range(3):
        for d in (1, 3, 2):
            tok_copy(t, d).start()
        tok_local(t).start()

    def z_copy(buf, s, r, d):
        return remote(
            buf.at[chip, c], buf.at[chip, c], s.at[d], r.at[d], wide_1=lax.rem(z + d, NZ)
        )

    def block_of(d):
        return x * NZ + lax.rem(z + NZ - d, NZ)

    def x_copy(buf, s, r, e, d):
        b = block_of(d)
        return remote(
            buf.at[b, c], buf.at[b, c], s.at[e, d], r.at[e, d], wide_0=lax.rem(x + e, NX)
        )

    def c_copy(buf, s, r, e):
        first = pl.multiple_of(lax.rem(x + NX - e, NX) * NZ, NZ)
        part = buf.at[pl.ds(first, NZ), c]
        return remote(part, part, s.at[e], r.at[e], wide_2=other)

    def gather(buf, z_s, z_r, x_s, x_r, c_s, c_r):
        for d in range(1, NZ // 2):
            z_copy(buf, z_s, z_r, d).start()
            z_copy(buf, z_s, z_r, NZ - d).start()
        z_copy(buf, z_s, z_r, NZ // 2).start()

        def forward(d):
            for e in (1, 3, 2):
                x_copy(buf, x_s, x_r, e, d).start()

        forward(0)

        def relay(d):
            b = block_of(d)
            remote(buf.at[b, c], buf.at[b, c], z_s.at[d], z_r.at[d], wide_1=z).wait_recv()
            forward(d)

        def relay_pair(d):
            relay(d)
            relay(NZ - d)

        loop(NZ // 2, relay_pair, 1)
        relay(NZ // 2)
        c_copy(buf, c_s, c_r, 0).start()
        for e in (1, 3, 2):

            def landed(d, e=e):
                b = lax.rem(x + NX - e, NX) * NZ + lax.rem(z + NZ - d, NZ)
                remote(
                    buf.at[b, c], buf.at[b, c], x_s.at[e, d], x_r.at[e, d], wide_0=x
                ).wait_recv()

            loop(NZ, landed)
            c_copy(buf, c_s, c_r, e).start()
        for e in range(NX):
            first = pl.multiple_of(lax.rem(x + NX - e, NX) * NZ, NZ)
            part = buf.at[pl.ds(first, NZ), other]
            remote(part, part, c_s.at[e], c_r.at[e], wide_2=other).wait_recv()

    def gather_sent(buf, z_s, z_r, x_s, x_r, c_s, c_r):
        def far(d):
            z_copy(buf, z_s, z_r, d).wait_send()

        loop(NZ, far, 1)

        def near(d):
            for e in range(1, NX):
                x_copy(buf, x_s, x_r, e, d).wait_send()

        loop(NZ, near)
        for e in range(NX):
            c_copy(buf, c_s, c_r, e).wait_send()

    swap.wait_recv()
    mine, theirs = ex[...], exr[...]
    first = c == 0
    rows8 = jnp.concatenate(
        [jnp.where(first, mine, theirs), jnp.where(first, theirs, mine)], axis=1
    )
    half = jnp.where(first, rows8[:, :, :HALF], rows8[:, :, HALF:])
    wbuf[chip, c] = half[:3].astype(BF16)
    mhalf[...] = half[3:]
    gather(wbuf, wz_s, wz_r, wx_s, wx_r, wc_s, wc_r)

    def square(i):
        r = pl.ds(pl.multiple_of(i * TOK, TOK), TOK)
        b = pl.ds(pl.multiple_of(i * NZ, NZ), NZ)
        for t in range(3):
            for h in range(2):
                part = wbuf[b, h, t].astype(F32).reshape(TOK, HALF)
                w2[t, r, h * HALF : (h + 1) * HALF] = part.astype(BF16)

    loop(4, square)
    tok_wait(0)
    tok_wait(1)

    kt[...] = kh[...].T

    def back(i):
        r = pl.ds(pl.multiple_of(i * TOK, TOK), TOK)
        kb = kh[r]
        pre_gate = mm(kb, w2[0])
        pre_up = mm(kb, w2[1])
        d_hidden = -nt(vh[r], w2[2])
        sig = jax.nn.sigmoid(pre_gate)
        activ = pre_gate * sig
        hid[r] = (activ * pre_up).astype(BF16)
        dg[r] = (d_hidden * pre_up * (sig * (1.0 + pre_gate * (1.0 - sig)))).astype(BF16)
        du[r] = (d_hidden * activ).astype(BF16)

    loop(4, back)
    ht[...] = hid[...].T

    def g_copy(b):
        return remote(gsend.at[b], grecv.at[b], gs_s.at[b], gs_r.at[b], wide_2=other)

    def grad(i):
        b = lax.rem(x + 1 + i, NX)
        r = pl.ds(pl.multiple_of(b * TOK, TOK), TOK)
        kb = kt[r]
        hb = ht[r]
        for t, g in enumerate((mm(kb, dg[...]), mm(kb, du[...]), -mm(hb, vh[...]))):
            own[b, t] = jnp.where(first, g[:, :HALF], g[:, HALF:])
            gsend[b, t] = jnp.where(first, g[:, HALF:], g[:, :HALF]).astype(BF16)
        g_copy(b).start()

    loop(NX, grad)

    def pair(i):
        b = lax.rem(x + 1 + i, NX)
        g_copy(b).wait_recv()
        for t in range(3):
            for j in range(4):
                total = own[b, t, j * 32 : (j + 1) * 32] + grecv[b, t, j * 32 : (j + 1) * 32].astype(F32)
                xs[b, j, t] = total.astype(BF16)

    loop(NX, pair)

    def part_of(j):
        return lax.rem(lax.div(z, 4) + 2 + j, 4)

    def rx_copy(j, e):
        to = lax.rem(x + e, NX)
        p = part_of(j)
        return remote(xs.at[to, p], xr.at[e, p], rx_s.at[e, p], rx_r.at[e, p], wide_0=to)

    def rx_start(j):
        for e in (1, 3, 2):
            rx_copy(j, e).start()

    loop(4, rx_start)

    tok_wait(2)
    gains = gain[:, cols(y)]
    e0 = lengths[0, 0]
    e1 = e0 + lengths[0, 1]
    e2 = e1 + lengths[0, 2]

    def ids(pos):
        return (
            (pos >= e0).astype(jnp.int32) + (pos >= e1).astype(jnp.int32) + (pos >= e2).astype(jnp.int32)
        )

    def attend(i):
        r = pl.ds(pl.multiple_of(i * TOK, TOK), TOK)
        scores = nt(qh[r], kh[...]) * (HEAD**-0.5)
        qid = ids(lax.broadcasted_iota(jnp.int32, (TOK, GROUP), 0) + i * TOK)
        kid = ids(lax.broadcasted_iota(jnp.int32, (TOK, GROUP), 1))
        scores = jnp.where(qid == kid, scores, -1e30)
        expo = jnp.exp(scores - jnp.max(scores, axis=-1, keepdims=True))
        probs = (expo / jnp.sum(expo, axis=-1, keepdims=True)).astype(BF16)
        view[r] = rms(mm(probs, vh[...]), gains).astype(BF16)

    loop(4, attend)

    def rz_copy(to):
        return remote(zs.at[to], zr.at[z], rz_s.at[to], rz_r.at[z], wide_1=to)

    def fold(j):
        p = part_of(j)
        for e in range(1, NX):
            remote(xs.at[x, p], xr.at[e, p], rx_s.at[e, p], rx_r.at[e, p], wide_0=x).wait_recv()
        total = xs[x, p].astype(F32)
        for e in range(1, NX):
            total = total + xr[e, p].astype(F32)
        for t in range(4):
            zs[p * 4 + t] = total[:, t * 8 : (t + 1) * 8].astype(BF16)
        for t in range(4):

            @pl.when(p * 4 + t != z)
            def _():
                rz_copy(p * 4 + t).start()

    loop(4, fold)
    zr[z] = zs[z]
    gather_sent(wbuf, wz_s, wz_r, wx_s, wx_r, wc_s, wc_r)

    def summed(d, total):
        frm = lax.rem(z + NZ - d, NZ)
        remote(zs.at[frm], zr.at[frm], rz_s.at[frm], rz_r.at[frm], wide_1=frm).wait_recv()
        return total + zr[frm].astype(F32)

    total = lax.fori_loop(1, NZ, summed, zr[z].astype(F32))
    mbuf[chip, c] = (momentum_decay * mhalf[...] + total * TOKENS**-0.5).astype(BF16)
    gather(mbuf, mz_s, mz_r, mx_s, mx_r, mc_s, mc_r)

    def squares(i, sums):
        b = pl.ds(pl.multiple_of(i * NZ, NZ), NZ)
        return tuple(
            s + jnp.sum(jnp.square(mbuf[b, 0, t].astype(F32)) + jnp.square(mbuf[b, 1, t].astype(F32)), axis=0)
            for t, s in enumerate(sums)
        )

    blank = jnp.zeros((8, HALF), F32)
    sums = lax.fori_loop(0, NX, squares, (blank, blank, blank))
    steps = tuple(
        step_size * lax.rsqrt(jnp.sum(jnp.sum(s, axis=1, keepdims=True), axis=0, keepdims=True) / HEAD**2 + epsilon)
        for s in sums
    )

    def moved_rows(w0, w1, m0, m1, step):
        v0 = w0 - m0 * step
        v1 = w1 - m1 * step
        before = jnp.sum(w0 * w0 + w1 * w1, axis=-1, keepdims=True) + epsilon
        after = jnp.sum(v0 * v0 + v1 * v1, axis=-1, keepdims=True) + epsilon
        ratio = jnp.sqrt(before) / jnp.sqrt(after)
        return v0 * ratio, v1 * ratio

    def renew(i):
        r = pl.ds(pl.multiple_of(i * TOK, TOK), TOK)
        b = pl.ds(pl.multiple_of(i * NZ, NZ), NZ)
        for t in range(3):
            parts = moved_rows(
                *(
                    buf[b, h, t].astype(F32).reshape(TOK, HALF)
                    for buf in (wbuf, mbuf)
                    for h in range(2)
                ),
                steps[t],
            )
            for h in range(2):
                n2[t, r, h * HALF : (h + 1) * HALF] = parts[h].astype(BF16)

    loop(4, renew)
    for d in range(1, NY):
        tok_copy(2, d).wait_send()

    def o_copy(i):
        to = lax.rem(y + 1 + i, NY)
        return remote(oblk.at[i], out.at[:, cols(y)], o_s.at[i], o_r.at[i], narrow=to)

    def apply(i):
        r = rows(lax.rem(y + 1 + i, NY))
        qb = qh[r]
        pre_gate = mm(qb, n2[0])
        pre_up = mm(qb, n2[1])
        hidden = (pre_gate * jax.nn.sigmoid(pre_gate) * pre_up).astype(BF16)
        fast = rms(mm(hidden, n2[2]), gains).astype(BF16)
        oblk[i] = (view[r].astype(F32) + fast.astype(F32)).astype(BF16)

        @pl.when(i < NY - 1)
        def _():
            o_copy(i).start()

    loop(NY, apply)
    keep = pltpu.make_async_copy(oblk.at[NY - 1], out.at[:, cols(y)], o_own)
    keep.start()

    for t, (new, mom) in enumerate(((ng, og), (nu, ou), (nd, od))):
        m0, m1 = mbuf[chip, 0, t].astype(F32), mbuf[chip, 1, t].astype(F32)
        parts = moved_rows(wbuf[chip, 0, t].astype(F32), wbuf[chip, 1, t].astype(F32), m0, m1, steps[t])
        whole = jnp.concatenate(parts, axis=1)
        new[0] = jnp.where(first, whole[:4], whole[4:]).astype(BF16)
        whole = jnp.concatenate([m0, m1], axis=1)
        mom[0] = jnp.where(first, whole[:4], whole[4:])

    swap.wait_send()
    for t in range(2):
        for d in range(1, NY):
            tok_copy(t, d).wait_send()
    for b in range(NX):
        g_copy(b).wait_send()
    for j in range(4):
        for e in range(1, NX):
            rx_copy(j, e).wait_send()

    def z_sent(d):
        rz_copy(lax.rem(z + d, NZ)).wait_send()

    loop(NZ, z_sent, 1)
    gather_sent(mbuf, mz_s, mz_r, mx_s, mx_r, mc_s, mc_r)
    for i in range(NY - 1):
        frm = lax.rem(y + NY - 1 - i, NY)
        remote(oblk.at[i], out.at[:, cols(frm)], o_s.at[i], o_r.at[i], narrow=frm).wait()
    keep.wait()


def per_device(queries, keys, values, view_lengths, gain, *weights):
    vmem = pl.BlockSpec(memory_space=pltpu.VMEM)
    anywhere = pl.BlockSpec(memory_space=pl.ANY)
    dma = pltpu.SemaphoreType.DMA
    sq = (HEAD, HEAD)
    gather_sems = [dma((NZ,)), dma((NZ,)), dma((NX, NZ)), dma((NX, NZ)), dma((NX,)), dma((NX,))]
    return pl.pallas_call(
        kernel,
        out_shape=(
            jax.ShapeDtypeStruct(queries.shape, BF16),
            *(jax.ShapeDtypeStruct((1, 4, HEAD), BF16) for _ in range(3)),
            *(jax.ShapeDtypeStruct((1, 4, HEAD), F32) for _ in range(3)),
        ),
        in_specs=[anywhere] * 3 + [pl.BlockSpec(memory_space=pltpu.SMEM)] + [vmem] * 7,
        out_specs=(anywhere, *[vmem] * 6),
        scratch_shapes=[
            *[pltpu.VMEM(sq, BF16)] * 8,
            pltpu.VMEM((6, 4, HEAD), F32),
            pltpu.VMEM((6, 4, HEAD), F32),
            pltpu.VMEM((3, 8, HALF), F32),
            pltpu.VMEM((CHIPS, 2, 3, 8, HALF), BF16),
            pltpu.VMEM((3, HEAD, HEAD), BF16),
            pltpu.VMEM((NX, 3, TOK, HALF), F32),
            pltpu.VMEM((NX, 3, TOK, HALF), BF16),
            pltpu.VMEM((NX, 3, TOK, HALF), BF16),
            pltpu.VMEM((NX, 4, 3, 32, HALF), BF16),
            pltpu.VMEM((NX, 4, 3, 32, HALF), BF16),
            pltpu.VMEM((NZ, 3, 8, HALF), BF16),
            pltpu.VMEM((NZ, 3, 8, HALF), BF16),
            pltpu.VMEM((CHIPS, 2, 3, 8, HALF), BF16),
            pltpu.VMEM((3, HEAD, HEAD), BF16),
            pltpu.VMEM(sq, BF16),
            pltpu.VMEM((NY, TOK, HEAD), BF16),
            dma((3, NY)), dma((3, NY)), dma((3,)), dma((2,)),
            *gather_sems,
            *gather_sems,
            dma((NX,)), dma((NX,)), dma((NX, 4)), dma((NX, 4)), dma((NZ,)), dma((NZ,)),
            dma((NY,)), dma((NY,)), dma,
        ],
        compiler_params=pltpu.CompilerParams(
            collective_id=0, has_side_effects=True, vmem_limit_bytes=48 * 1024 * 1024
        ),
    )(queries, keys, values, view_lengths, gain.reshape(1, -1), *weights)


def solution(mesh):
    split = Mesh(
        mesh.devices.reshape(NX, NZ, 2, mesh.shape["narrow"]),
        ("wide_0", "wide_1", "wide_2", "narrow"),
    )
    rows = P("narrow", WIDE, None)
    return jax.shard_map(
        per_device,
        mesh=split,
        in_specs=(*[P(WIDE_NARROW, None)] * 3, P(WIDE, None), P(), *[rows] * 6),
        out_specs=(P(WIDE_NARROW, None), *[rows] * 6),
        check_vma=False,
    )
```

```python
import functools

import jax
import jax.numpy as jnp
from jax import lax
from jax.experimental import pallas as pl
from jax.experimental.pallas import tpu as pltpu
from jax.sharding import Mesh
from jax.sharding import PartitionSpec as P

WIDE = ("wide_0", "wide_1", "wide_2")
WIDE_NARROW = ("wide_0", "wide_1", "wide_2", "narrow")
MESH = pl.DeviceIdType.MESH

momentum_decay = 0.9
step_size = 0.02
epsilon = 1e-06

NX, NZ, NY = 4, 16, 4
NEAR = 4
HEAD = 512
HALF = 256
GROUP = 512
TOK = 128
CHIPS = NX * NZ
TOKENS = 65536
F32 = jnp.float32
BF16 = jnp.bfloat16


def nt(a, b):
    return lax.dot_general(a, b, (((1,), (1,)), ((), ())), preferred_element_type=F32)


def mm(a, b):
    return jnp.dot(a, b, preferred_element_type=F32)


def rms(field, gains):
    return field * lax.rsqrt(jnp.mean(field * field, axis=-1, keepdims=True) + epsilon) * gains


def remote(src, dst, send, recv, **where):
    return pltpu.make_async_remote_copy(
        src_ref=src, dst_ref=dst, send_sem=send, recv_sem=recv, device_id=where, device_id_type=MESH
    )


def loop(n, body, start=0):
    def step(i, carry):
        body(i)
        return carry

    lax.fori_loop(start, n, step, 0)


def kernel(
    q_in, k_in, v_in, lengths_in, gain_in, wg, wu, wd, mg, mu, md,
    out, new_out, mom_out,
    lengths, gain, wrow, newv, momv, small_sem,
    qh, kh, vh, kt, ht, hid, dg, du, ex, exr, mhalf, wbuf, w2, own, gsend, grecv,
    xs, xr, zs, zr, mbuf, n2, view, oblk,
    tok_send, tok_recv, tok_own, ex_sem, wz_s, wz_r, wx_s, wx_r, wc_s, wc_r,
    mz_s, mz_r, mx_s, mx_r, mc_s, mc_r, gs_s, gs_r, rx_s, rx_r, rz_s, rz_r, o_s, o_r, o_own,
):
    x = lax.axis_index("wide_0")
    z = lax.axis_index("wide_1")
    c = lax.axis_index("wide_2")
    y = lax.axis_index("narrow")
    chip = x * NZ + z
    other = 1 - c

    small = [pltpu.make_async_copy(w.at[0], wrow.at[t], small_sem.at[t]) for t, w in enumerate((wg, wu, wd))]
    small += [pltpu.make_async_copy(m.at[0], ex.at[3 + t], small_sem.at[3 + t]) for t, m in enumerate((mg, mu, md))]
    small += [
        pltpu.make_async_copy(lengths_in, lengths, small_sem.at[6]),
        pltpu.make_async_copy(gain_in, gain, small_sem.at[7]),
    ]
    for copy in small:
        copy.start()

    barrier = pltpu.get_barrier_semaphore()
    pl.semaphore_signal(barrier, inc=1, device_id={"wide_2": other}, device_id_type=MESH)
    for d in range(1, NY):
        pl.semaphore_signal(
            barrier, inc=1, device_id={"narrow": lax.rem(y + d, NY)}, device_id_type=MESH
        )
    for d in range(1, NX):
        pl.semaphore_signal(
            barrier, inc=1, device_id={"wide_0": lax.rem(x + d, NX)}, device_id_type=MESH
        )

    def greet(d):
        pl.semaphore_signal(
            barrier, inc=1, device_id={"wide_1": lax.rem(z + d, NZ)}, device_id_type=MESH
        )

    for d in range(1, NEAR + 1):
        greet(d)
        greet(NZ - d)
    for copy in small:
        copy.wait()
    ex[:3] = wrow[...].astype(F32)
    pl.semaphore_wait(barrier, NY - 1 + NX - 1 + 2 * NEAR + 1)

    def cols(who):
        return pl.ds(pl.multiple_of(who * HEAD, HEAD), HEAD)

    def rows(who):
        return pl.ds(pl.multiple_of(who * TOK, TOK), TOK)

    trio = ((k_in, kh), (v_in, vh), (q_in, qh))

    def tok_copy(t, d):
        src, dst = trio[t]
        to = lax.rem(y + d, NY)
        return remote(
            src.at[:, cols(to)], dst.at[rows(y)], tok_send.at[t, d], tok_recv.at[t, d], narrow=to
        )

    def tok_wait(t):
        src, dst = trio[t]
        for d in range(1, NY):
            frm = lax.rem(y + NY - d, NY)
            remote(
                src.at[:, cols(y)], dst.at[rows(frm)], tok_send.at[t, d], tok_recv.at[t, d], narrow=frm
            ).wait_recv()
        tok_local(t).wait()

    def tok_local(t):
        src, dst = trio[t]
        return pltpu.make_async_copy(src.at[:, cols(y)], dst.at[rows(y)], tok_own.at[t])

    swap = remote(ex, exr, ex_sem.at[0], ex_sem.at[1], wide_2=other)
    swap.start()
    for t in range(3):
        for d in (1, 3, 2):
            tok_copy(t, d).start()
        tok_local(t).start()

    def z_copy(buf, s, r, d):
        return remote(
            buf.at[chip, c], buf.at[chip, c], s.at[d], r.at[d], wide_1=lax.rem(z + d, NZ)
        )

    def block_of(d):
        return x * NZ + lax.rem(z + NZ - d, NZ)

    def x_copy(buf, s, r, e, d):
        b = block_of(d)
        return remote(
            buf.at[b, c], buf.at[b, c], s.at[e, d], r.at[e, d], wide_0=lax.rem(x + e, NX)
        )

    def z_relay(buf, s, r, via, d):
        hop = d - via if d <= NZ // 2 else NZ - (via - d)
        b = block_of(via)
        return remote(
            buf.at[b, c], buf.at[b, c], s.at[d], r.at[d], wide_1=lax.rem(z + hop, NZ)
        )

    def gather(buf, z_s, z_r, x_s, x_r, c_s, c_r):
        def forward(d):
            for e in (1, 3, 2):
                x_copy(buf, x_s, x_r, e, d).start()

        def landed(d):
            b = block_of(d)
            remote(buf.at[b, c], buf.at[b, c], z_s.at[d], z_r.at[d], wide_1=z).wait_recv()

        def across(b):
            remote(buf.at[b, c], buf.at[b, c], c_s, c_r, wide_2=other).start()

        for d in range(NEAR, 0, -1):
            z_copy(buf, z_s, z_r, d).start()
            z_copy(buf, z_s, z_r, NZ - d).start()
        forward(0)
        across(chip)
        for d in range(1, NEAR + 1):
            for o in (d, NZ - d):
                landed(o)
                if d == NEAR:
                    for n in range(NEAR, 0, -1):
                        if o == NEAR:
                            z_relay(buf, z_s, z_r, o, NEAR + n).start()
                        elif NEAR + n < NZ // 2:
                            z_relay(buf, z_s, z_r, o, NZ - NEAR - n).start()
                forward(o)
                across(block_of(o))
        for d in range(NEAR + 1, NZ // 2 + 1):
            for o in (d, NZ - d) if d < NZ // 2 else (d,):
                landed(o)
                forward(o)
                across(block_of(o))

        def arrived(d):
            for e in (1, 3, 2):
                b = lax.rem(x + NX - e, NX) * NZ + lax.rem(z + NZ - d, NZ)
                remote(
                    buf.at[b, c], buf.at[b, c], x_s.at[e, d], x_r.at[e, d], wide_0=x
                ).wait_recv()
                across(b)

        arrived(0)

        def arrived_pair(d):
            arrived(d)
            arrived(NZ - d)

        loop(NZ // 2, arrived_pair, 1)
        arrived(NZ // 2)
        remote(buf.at[:, other], buf.at[:, other], c_s, c_r, wide_2=other).wait_recv()

    def gather_sent(buf, z_s, z_r, x_s, x_r, c_s, c_r):
        def far(d):
            z_copy(buf, z_s, z_r, d).wait_send()

        loop(NZ, far, 1)

        def near(d):
            for e in range(1, NX):
                x_copy(buf, x_s, x_r, e, d).wait_send()

        loop(NZ, near)
        remote(buf.at[:, c], buf.at[:, c], c_s, c_r, wide_2=other).wait_send()

    swap.wait_recv()
    mine, theirs = ex[...], exr[...]
    first = c == 0
    rows8 = jnp.concatenate(
        [jnp.where(first, mine, theirs), jnp.where(first, theirs, mine)], axis=1
    )
    half = jnp.where(first, rows8[:, :, :HALF], rows8[:, :, HALF:])
    wbuf[chip, c] = half[:3].astype(BF16)
    mhalf[...] = half[3:]
    gather(wbuf, wz_s, wz_r, wx_s, wx_r, wc_s, wc_r)

    def square(i):
        r = pl.ds(pl.multiple_of(i * TOK, TOK), TOK)
        b = pl.ds(pl.multiple_of(i * NZ, NZ), NZ)
        for t in range(3):
            for h in range(2):
                part = wbuf[b, h, t].astype(F32).reshape(TOK, HALF)
                w2[t, r, h * HALF : (h + 1) * HALF] = part.astype(BF16)

    loop(4, square)
    tok_wait(0)
    tok_wait(1)

    kt[...] = kh[...].T

    def back(i):
        r = pl.ds(pl.multiple_of(i * TOK, TOK), TOK)
        kb = kh[r]
        pre_gate = mm(kb, w2[0])
        pre_up = mm(kb, w2[1])
        d_hidden = -nt(vh[r], w2[2])
        sig = jax.nn.sigmoid(pre_gate)
        activ = pre_gate * sig
        hid[r] = (activ * pre_up).astype(BF16)
        dg[r] = (d_hidden * pre_up * (sig * (1.0 + pre_gate * (1.0 - sig)))).astype(BF16)
        du[r] = (d_hidden * activ).astype(BF16)

    loop(4, back)
    ht[...] = hid[...].T

    def g_copy(b):
        return remote(gsend.at[b], grecv.at[b], gs_s.at[b], gs_r.at[b], wide_2=other)

    def grad(i):
        b = lax.rem(x + 1 + i, NX)
        r = pl.ds(pl.multiple_of(b * TOK, TOK), TOK)
        kb = kt[r]
        hb = ht[r]
        for t, g in enumerate((mm(kb, dg[...]), mm(kb, du[...]), -mm(hb, vh[...]))):
            own[b, t] = jnp.where(first, g[:, :HALF], g[:, HALF:])
            gsend[b, t] = jnp.where(first, g[:, HALF:], g[:, :HALF]).astype(BF16)
        g_copy(b).start()

    loop(NX, grad)

    def pair(i):
        b = lax.rem(x + 1 + i, NX)
        g_copy(b).wait_recv()
        for t in range(3):
            for j in range(4):
                total = own[b, t, j * 32 : (j + 1) * 32] + grecv[b, t, j * 32 : (j + 1) * 32].astype(F32)
                xs[b, j, t] = total.astype(BF16)

    loop(NX, pair)

    def part_of(j):
        return lax.rem(lax.div(z, 4) + 2 + j, 4)

    def rx_copy(j, e):
        to = lax.rem(x + e, NX)
        p = part_of(j)
        return remote(xs.at[to, p], xr.at[e, p], rx_s.at[e, p], rx_r.at[e, p], wide_0=to)

    def rx_start(j):
        for e in (1, 3, 2):
            rx_copy(j, e).start()

    loop(4, rx_start)

    tok_wait(2)
    gains = gain[:, cols(y)]
    e0 = lengths[0, 0]
    e1 = e0 + lengths[0, 1]
    e2 = e1 + lengths[0, 2]

    def ids(pos):
        return (
            (pos >= e0).astype(jnp.int32) + (pos >= e1).astype(jnp.int32) + (pos >= e2).astype(jnp.int32)
        )

    def attend(i):
        r = pl.ds(pl.multiple_of(i * TOK, TOK), TOK)
        scores = nt(qh[r], kh[...]) * (HEAD**-0.5)
        qid = ids(lax.broadcasted_iota(jnp.int32, (TOK, GROUP), 0) + i * TOK)
        kid = ids(lax.broadcasted_iota(jnp.int32, (TOK, GROUP), 1))
        scores = jnp.where(qid == kid, scores, -1e30)
        expo = jnp.exp(scores - jnp.max(scores, axis=-1, keepdims=True))
        probs = (expo / jnp.sum(expo, axis=-1, keepdims=True)).astype(BF16)
        view[r] = rms(mm(probs, vh[...]), gains).astype(BF16)

    loop(4, attend)

    def rz_copy(to):
        return remote(zs.at[to], zr.at[z], rz_s.at[to], rz_r.at[z], wide_1=to)

    def fold(j):
        p = part_of(j)
        for e in range(1, NX):
            remote(xs.at[x, p], xr.at[e, p], rx_s.at[e, p], rx_r.at[e, p], wide_0=x).wait_recv()
        total = xs[x, p].astype(F32)
        for e in range(1, NX):
            total = total + xr[e, p].astype(F32)
        for t in range(4):
            zs[p * 4 + t] = total[:, t * 8 : (t + 1) * 8].astype(BF16)
        for t in range(4):

            @pl.when(p * 4 + t != z)
            def _():
                rz_copy(p * 4 + t).start()

    loop(4, fold)
    zr[z] = zs[z]
    gather_sent(wbuf, wz_s, wz_r, wx_s, wx_r, wc_s, wc_r)

    def summed(d, total):
        frm = lax.rem(z + NZ - d, NZ)
        remote(zs.at[frm], zr.at[frm], rz_s.at[frm], rz_r.at[frm], wide_1=frm).wait_recv()
        return total + zr[frm].astype(F32)

    total = lax.fori_loop(1, NZ, summed, zr[z].astype(F32))
    mbuf[chip, c] = (momentum_decay * mhalf[...] + total * TOKENS**-0.5).astype(BF16)
    gather(mbuf, mz_s, mz_r, mx_s, mx_r, mc_s, mc_r)

    def squares(i, sums):
        b = pl.ds(pl.multiple_of(i * NZ, NZ), NZ)
        return tuple(
            s + jnp.sum(jnp.square(mbuf[b, 0, t].astype(F32)) + jnp.square(mbuf[b, 1, t].astype(F32)), axis=0)
            for t, s in enumerate(sums)
        )

    blank = jnp.zeros((8, HALF), F32)
    sums = lax.fori_loop(0, NX, squares, (blank, blank, blank))
    steps = tuple(
        step_size * lax.rsqrt(jnp.sum(jnp.sum(s, axis=1, keepdims=True), axis=0, keepdims=True) / HEAD**2 + epsilon)
        for s in sums
    )

    def moved_rows(w0, w1, m0, m1, step):
        v0 = w0 - m0 * step
        v1 = w1 - m1 * step
        before = jnp.sum(w0 * w0 + w1 * w1, axis=-1, keepdims=True) + epsilon
        after = jnp.sum(v0 * v0 + v1 * v1, axis=-1, keepdims=True) + epsilon
        ratio = jnp.sqrt(before) / jnp.sqrt(after)
        return v0 * ratio, v1 * ratio

    def renew(i):
        r = pl.ds(pl.multiple_of(i * TOK, TOK), TOK)
        b = pl.ds(pl.multiple_of(i * NZ, NZ), NZ)
        for t in range(3):
            parts = moved_rows(
                *(
                    buf[b, h, t].astype(F32).reshape(TOK, HALF)
                    for buf in (wbuf, mbuf)
                    for h in range(2)
                ),
                steps[t],
            )
            for h in range(2):
                n2[t, r, h * HALF : (h + 1) * HALF] = parts[h].astype(BF16)

    loop(4, renew)
    for d in range(1, NY):
        tok_copy(2, d).wait_send()

    def o_copy(i):
        to = lax.rem(y + 1 + i, NY)
        return remote(oblk.at[i], out.at[:, cols(y)], o_s.at[i], o_r.at[i], narrow=to)

    def apply(i):
        r = rows(lax.rem(y + 1 + i, NY))
        qb = qh[r]
        pre_gate = mm(qb, n2[0])
        pre_up = mm(qb, n2[1])
        hidden = (pre_gate * jax.nn.sigmoid(pre_gate) * pre_up).astype(BF16)
        fast = rms(mm(hidden, n2[2]), gains).astype(BF16)
        oblk[i] = (view[r].astype(F32) + fast.astype(F32)).astype(BF16)

        @pl.when(i < NY - 1)
        def _():
            o_copy(i).start()

    loop(NY, apply)
    keep = pltpu.make_async_copy(oblk.at[NY - 1], out.at[:, cols(y)], o_own)
    keep.start()

    for t in range(3):
        m0, m1 = mbuf[chip, 0, t].astype(F32), mbuf[chip, 1, t].astype(F32)
        parts = moved_rows(wbuf[chip, 0, t].astype(F32), wbuf[chip, 1, t].astype(F32), m0, m1, steps[t])
        whole = jnp.concatenate(parts, axis=1)
        newv[t] = jnp.where(first, whole[:4], whole[4:]).astype(BF16)
        whole = jnp.concatenate([m0, m1], axis=1)
        momv[t] = jnp.where(first, whole[:4], whole[4:])
    done = [
        pltpu.make_async_copy(newv, new_out, small_sem.at[0]),
        pltpu.make_async_copy(momv, mom_out, small_sem.at[1]),
    ]
    for copy in done:
        copy.start()

    swap.wait_send()
    for t in range(2):
        for d in range(1, NY):
            tok_copy(t, d).wait_send()
    for b in range(NX):
        g_copy(b).wait_send()
    for j in range(4):
        for e in range(1, NX):
            rx_copy(j, e).wait_send()

    def z_sent(d):
        rz_copy(lax.rem(z + d, NZ)).wait_send()

    loop(NZ, z_sent, 1)
    gather_sent(mbuf, mz_s, mz_r, mx_s, mx_r, mc_s, mc_r)
    for i in range(NY - 1):
        frm = lax.rem(y + NY - 1 - i, NY)
        remote(oblk.at[i], out.at[:, cols(frm)], o_s.at[i], o_r.at[i], narrow=frm).wait()
    keep.wait()
    for copy in done:
        copy.wait()


def deliver(out_in, new_in, mom_in, out, ng, nu, nd, og, ou, od, outv, newv, momv, sems):
    quarter = TOK // 4
    parts = [pl.ds(i * quarter, quarter) for i in range(4)]
    get = [pltpu.make_async_copy(new_in, newv, sems.at[0]), pltpu.make_async_copy(mom_in, momv, sems.at[1])]
    get += [pltpu.make_async_copy(out_in.at[p], outv.at[p], sems.at[2 + i]) for i, p in enumerate(parts)]
    put = [
        [pltpu.make_async_copy(newv.at[t], o.at[0], sems.at[6 + t]) for t, o in enumerate((ng, nu, nd))],
        [pltpu.make_async_copy(momv.at[t], o.at[0], sems.at[9 + t]) for t, o in enumerate((og, ou, od))],
        *([pltpu.make_async_copy(outv.at[p], out.at[p], sems.at[12 + i])] for i, p in enumerate(parts)),
    ]
    for copy in get:
        copy.start()
    for copy, then in zip(get, put):
        copy.wait()
        for other in then:
            other.start()
    for then in put:
        for other in then:
            other.wait()


def per_device(queries, keys, values, view_lengths, gain, *weights):
    hbm = pl.BlockSpec(memory_space=pltpu.HBM)
    dma = pltpu.SemaphoreType.DMA
    sq = (HEAD, HEAD)
    row = (4, HEAD)
    gather_sems = [dma((NZ,)), dma((NZ,)), dma((NX, NZ)), dma((NX, NZ)), dma, dma]
    parts = pl.pallas_call(
        kernel,
        out_shape=(
            jax.ShapeDtypeStruct(queries.shape, BF16),
            jax.ShapeDtypeStruct((3, *row), BF16),
            jax.ShapeDtypeStruct((3, *row), F32),
        ),
        in_specs=[hbm] * 11,
        out_specs=(hbm,) * 3,
        scratch_shapes=[
            pltpu.SMEM(view_lengths.shape, jnp.int32),
            pltpu.VMEM((1, gain.shape[0]), F32),
            pltpu.VMEM((3, *row), BF16),
            pltpu.VMEM((3, *row), BF16),
            pltpu.VMEM((3, *row), F32),
            dma((8,)),
            *[pltpu.VMEM(sq, BF16)] * 8,
            pltpu.VMEM((6, *row), F32),
            pltpu.VMEM((6, *row), F32),
            pltpu.VMEM((3, 8, HALF), F32),
            pltpu.VMEM((CHIPS, 2, 3, 8, HALF), BF16),
            pltpu.VMEM((3, HEAD, HEAD), BF16),
            pltpu.VMEM((NX, 3, TOK, HALF), F32),
            pltpu.VMEM((NX, 3, TOK, HALF), BF16),
            pltpu.VMEM((NX, 3, TOK, HALF), BF16),
            pltpu.VMEM((NX, 4, 3, 32, HALF), BF16),
            pltpu.VMEM((NX, 4, 3, 32, HALF), BF16),
            pltpu.VMEM((NZ, 3, 8, HALF), BF16),
            pltpu.VMEM((NZ, 3, 8, HALF), BF16),
            pltpu.VMEM((CHIPS, 2, 3, 8, HALF), BF16),
            pltpu.VMEM((3, HEAD, HEAD), BF16),
            pltpu.VMEM(sq, BF16),
            pltpu.VMEM((NY, TOK, HEAD), BF16),
            dma((3, NY)), dma((3, NY)), dma((3,)), dma((2,)),
            *gather_sems,
            *gather_sems,
            dma((NX,)), dma((NX,)), dma((NX, 4)), dma((NX, 4)), dma((NZ,)), dma((NZ,)),
            dma((NY,)), dma((NY,)), dma,
        ],
        compiler_params=pltpu.CompilerParams(
            collective_id=0, has_side_effects=True, vmem_limit_bytes=67_043_328
        ),
    )(queries, keys, values, view_lengths, gain.reshape(1, -1), *weights)
    return pl.pallas_call(
        deliver,
        out_shape=(
            jax.ShapeDtypeStruct(queries.shape, BF16),
            *[jax.ShapeDtypeStruct((1, *row), BF16)] * 3,
            *[jax.ShapeDtypeStruct((1, *row), F32)] * 3,
        ),
        in_specs=[hbm] * 3,
        out_specs=(hbm,) * 7,
        scratch_shapes=[
            pltpu.VMEM(queries.shape, BF16),
            pltpu.VMEM((3, *row), BF16),
            pltpu.VMEM((3, *row), F32),
            dma((16,)),
        ],
        compiler_params=pltpu.CompilerParams(vmem_limit_bytes=67_043_328),
    )(*parts)


def solution(mesh):
    split = Mesh(
        mesh.devices.reshape(NX, NZ, 2, mesh.shape["narrow"]),
        ("wide_0", "wide_1", "wide_2", "narrow"),
    )
    rows = P("narrow", WIDE, None)
    return jax.shard_map(
        per_device,
        mesh=split,
        in_specs=(*[P(WIDE_NARROW, None)] * 3, P(WIDE, None), P(), *[rows] * 6),
        out_specs=(P(WIDE_NARROW, None), *[rows] * 6),
        check_vma=False,
    )
```

```python
import functools

import jax
import jax.numpy as jnp
from jax import lax
from jax.experimental import pallas as pl
from jax.experimental.pallas import tpu as pltpu
from jax.sharding import Mesh
from jax.sharding import PartitionSpec as P

WIDE = ("wide_0", "wide_1", "wide_2")
WIDE_NARROW = ("wide_0", "wide_1", "wide_2", "narrow")
MESH = pl.DeviceIdType.MESH

momentum_decay = 0.9
step_size = 0.02
epsilon = 1e-06

NX, NZ, NY = 4, 16, 4
NEAR = 4
HEAD = 512
HALF = 256
GROUP = 512
TOK = 128
CHIPS = NX * NZ
TOKENS = 65536
F32 = jnp.float32
BF16 = jnp.bfloat16


def nt(a, b):
    return lax.dot_general(a, b, (((1,), (1,)), ((), ())), preferred_element_type=F32)


def mm(a, b):
    return jnp.dot(a, b, preferred_element_type=F32)


def rms(field, gains):
    return field * lax.rsqrt(jnp.mean(field * field, axis=-1, keepdims=True) + epsilon) * gains


def remote(src, dst, send, recv, **where):
    return pltpu.make_async_remote_copy(
        src_ref=src, dst_ref=dst, send_sem=send, recv_sem=recv, device_id=where, device_id_type=MESH
    )


def loop(n, body, start=0):
    def step(i, carry):
        body(i)
        return carry

    lax.fori_loop(start, n, step, 0)


def kernel(
    q_in, k_in, v_in, lengths_in, gain_in, wg, wu, wd, mg, mu, md,
    out, new_out, mom_out,
    lengths, gain, wrow, newv, momv, small_sem,
    qh, kh, vh, kt, ht, hid, dg, du, ex, exr, mhalf, wbuf, w2, own, gsend, grecv,
    xs, xr, zs, zr, mbuf, n2, view, oblk,
    tok_send, tok_recv, tok_own, ex_sem, wz_s, wz_r, wx_s, wx_r, wc_s, wc_r,
    mz_s, mz_r, mx_s, mx_r, mc_s, mc_r, gs_s, gs_r, rx_s, rx_r, rz_s, rz_r, o_s, o_r, o_own,
):
    x = lax.axis_index("wide_0")
    z = lax.axis_index("wide_1")
    c = lax.axis_index("wide_2")
    y = lax.axis_index("narrow")
    chip = x * NZ + z
    other = 1 - c

    small = [pltpu.make_async_copy(w.at[0], wrow.at[t], small_sem.at[t]) for t, w in enumerate((wg, wu, wd))]
    small += [pltpu.make_async_copy(m.at[0], ex.at[3 + t], small_sem.at[3 + t]) for t, m in enumerate((mg, mu, md))]
    small += [
        pltpu.make_async_copy(lengths_in, lengths, small_sem.at[6]),
        pltpu.make_async_copy(gain_in, gain, small_sem.at[7]),
    ]
    for copy in small:
        copy.start()

    barrier = pltpu.get_barrier_semaphore()
    pl.semaphore_signal(barrier, inc=1, device_id={"wide_2": other}, device_id_type=MESH)
    for d in range(1, NY):
        pl.semaphore_signal(
            barrier, inc=1, device_id={"narrow": lax.rem(y + d, NY)}, device_id_type=MESH
        )
    for d in range(1, NX):
        pl.semaphore_signal(
            barrier, inc=1, device_id={"wide_0": lax.rem(x + d, NX)}, device_id_type=MESH
        )

    def greet(d):
        pl.semaphore_signal(
            barrier, inc=1, device_id={"wide_1": lax.rem(z + d, NZ)}, device_id_type=MESH
        )

    for d in range(1, NEAR + 1):
        greet(d)
        greet(NZ - d)
    for copy in small:
        copy.wait()
    ex[:3] = wrow[...].astype(F32)
    pl.semaphore_wait(barrier, NY - 1 + NX - 1 + 2 * NEAR + 1)

    def cols(who):
        return pl.ds(pl.multiple_of(who * HEAD, HEAD), HEAD)

    def rows(who):
        return pl.ds(pl.multiple_of(who * TOK, TOK), TOK)

    trio = ((k_in, kh), (v_in, vh), (q_in, qh))

    def tok_copy(t, d):
        src, dst = trio[t]
        to = lax.rem(y + d, NY)
        return remote(
            src.at[:, cols(to)], dst.at[rows(y)], tok_send.at[t, d], tok_recv.at[t, d], narrow=to
        )

    def tok_wait(t):
        src, dst = trio[t]
        for d in range(1, NY):
            frm = lax.rem(y + NY - d, NY)
            remote(
                src.at[:, cols(y)], dst.at[rows(frm)], tok_send.at[t, d], tok_recv.at[t, d], narrow=frm
            ).wait_recv()
        tok_local(t).wait()

    def tok_local(t):
        src, dst = trio[t]
        return pltpu.make_async_copy(src.at[:, cols(y)], dst.at[rows(y)], tok_own.at[t])

    swap = remote(ex, exr, ex_sem.at[0], ex_sem.at[1], wide_2=other)
    swap.start()
    for t in range(3):
        for d in (1, 3, 2):
            tok_copy(t, d).start()
        tok_local(t).start()

    def z_copy(buf, s, r, d):
        return remote(
            buf.at[chip, c], buf.at[chip, c], s.at[d], r.at[d], wide_1=lax.rem(z + d, NZ)
        )

    def block_of(d):
        return x * NZ + lax.rem(z + NZ - d, NZ)

    def x_copy(buf, s, r, e, d):
        b = block_of(d)
        return remote(
            buf.at[b, c], buf.at[b, c], s.at[e, d], r.at[e, d], wide_0=lax.rem(x + e, NX)
        )

    def z_relay(buf, s, r, via, d):
        hop = d - via if d <= NZ // 2 else NZ - (via - d)
        b = block_of(via)
        return remote(
            buf.at[b, c], buf.at[b, c], s.at[d], r.at[d], wide_1=lax.rem(z + hop, NZ)
        )

    def gather(buf, z_s, z_r, x_s, x_r, c_s, c_r, meanwhile=None):
        def forward(d, order=(1, 3, 2)):
            for e in order:
                x_copy(buf, x_s, x_r, e, d).start()

        def landed(d):
            b = block_of(d)
            remote(buf.at[b, c], buf.at[b, c], z_s.at[d], z_r.at[d], wide_1=z).wait_recv()

        def across(b):
            remote(buf.at[b, c], buf.at[b, c], c_s, c_r, wide_2=other).start()

        def arrived(d, onward=()):
            for e in (1, 3, 2):
                b = lax.rem(x + NX - e, NX) * NZ + lax.rem(z + NZ - d, NZ)
                remote(
                    buf.at[b, c], buf.at[b, c], x_s.at[e, d], x_r.at[e, d], wide_0=x
                ).wait_recv()
                for n in onward:
                    to = lax.rem(z + NZ + n - d, NZ)
                    remote(buf.at[b, c], buf.at[b, c], x_s.at[e, n], x_r.at[e, n], wide_1=to).start()
                across(b)

        for d in range(NEAR, 0, -1):
            z_copy(buf, z_s, z_r, d).start()
            z_copy(buf, z_s, z_r, NZ - d).start()
        forward(0)
        across(chip)
        for d in range(1, NEAR + 1):
            for o in (d, NZ - d):
                landed(o)
                if d == NEAR:
                    for n in range(NEAR, 0, -1):
                        if o == NEAR:
                            z_relay(buf, z_s, z_r, o, NEAR + n).start()
                        elif NEAR + n < NZ // 2:
                            z_relay(buf, z_s, z_r, o, NZ - NEAR - n).start()
                forward(o)
                across(block_of(o))
        arrived(0)
        arrived(4, (6, 5))
        arrived(12, (10, 11))
        for o in (7, 9, 8):
            landed(o)
            forward(o, (2, 1, 3))
            across(block_of(o))
        for o in (5, 11, 6, 10):
            landed(o)
            across(block_of(o))
        if meanwhile is not None:
            meanwhile()

        def arrived_pair(d):
            arrived(d)
            arrived(NZ - d)

        loop(NEAR, arrived_pair, 1)
        loop(NZ // 2, arrived_pair, NEAR + 1)
        arrived(NZ // 2)
        remote(buf.at[:, other], buf.at[:, other], c_s, c_r, wide_2=other).wait_recv()

    def gather_sent(buf, z_s, z_r, x_s, x_r, c_s, c_r):
        def far(d):
            z_copy(buf, z_s, z_r, d).wait_send()

        loop(NZ, far, 1)

        def near(d):
            for e in range(1, NX):
                x_copy(buf, x_s, x_r, e, d).wait_send()

        loop(NZ, near)
        remote(buf.at[:, c], buf.at[:, c], c_s, c_r, wide_2=other).wait_send()

    swap.wait_recv()
    mine, theirs = ex[...], exr[...]
    first = c == 0
    rows8 = jnp.concatenate(
        [jnp.where(first, mine, theirs), jnp.where(first, theirs, mine)], axis=1
    )
    half = jnp.where(first, rows8[:, :, :HALF], rows8[:, :, HALF:])
    wbuf[chip, c] = half[:3].astype(BF16)
    mhalf[...] = half[3:]

    def turn_keys():
        tok_wait(0)
        kt[...] = kh[...].T

    gather(wbuf, wz_s, wz_r, wx_s, wx_r, wc_s, wc_r, turn_keys)

    def square(i):
        r = pl.ds(pl.multiple_of(i * TOK, TOK), TOK)
        b = pl.ds(pl.multiple_of(i * NZ, NZ), NZ)
        for t in range(3):
            for h in range(2):
                part = wbuf[b, h, t].astype(F32).reshape(TOK, HALF)
                w2[t, r, h * HALF : (h + 1) * HALF] = part.astype(BF16)

    loop(4, square)
    tok_wait(1)


    def back(i):
        r = pl.ds(pl.multiple_of(i * TOK, TOK), TOK)
        kb = kh[r]
        pre_gate = mm(kb, w2[0])
        pre_up = mm(kb, w2[1])
        d_hidden = -nt(vh[r], w2[2])
        sig = jax.nn.sigmoid(pre_gate)
        activ = pre_gate * sig
        hid[r] = (activ * pre_up).astype(BF16)
        dg[r] = (d_hidden * pre_up * (sig * (1.0 + pre_gate * (1.0 - sig)))).astype(BF16)
        du[r] = (d_hidden * activ).astype(BF16)

    loop(4, back)
    ht[...] = hid[...].T

    def g_copy(b):
        return remote(gsend.at[b], grecv.at[b], gs_s.at[b], gs_r.at[b], wide_2=other)

    def part_of(j):
        return lax.rem(lax.div(z, 4) + 2 + j + lax.div(j * (j - 1), 2), 4)

    def grad(j):
        p = part_of(j)
        quarter = [pl.ds(pl.multiple_of(b * TOK + p * 32, 32), 32) for b in range(NX)]
        kb = jnp.concatenate([kt[r] for r in quarter], axis=0)
        hb = jnp.concatenate([ht[r] for r in quarter], axis=0)
        for t, g in enumerate((mm(kb, dg[...]), mm(kb, du[...]), -mm(hb, vh[...]))):
            keep = jnp.where(first, g[:, :HALF], g[:, HALF:])
            give = jnp.where(first, g[:, HALF:], g[:, :HALF]).astype(BF16)
            for b in range(NX):
                own[p, b, t] = keep[b * 32 : (b + 1) * 32]
                gsend[p, b, t] = give[b * 32 : (b + 1) * 32]
        g_copy(p).start()

    def rx_copy(j, e):
        to = lax.rem(x + e, NX)
        p = part_of(j)
        return remote(xs.at[to, p], xr.at[e, p], rx_s.at[e, p], rx_r.at[e, p], wide_0=to)

    def pair(j):
        p = part_of(j)
        g_copy(p).wait_recv()
        for b in range(NX):
            for t in range(3):
                xs[b, p, t] = (own[p, b, t] + grecv[p, b, t].astype(F32)).astype(BF16)
        for e in (1, 3, 2):
            rx_copy(j, e).start()

    def grad_and_pair(j):
        grad(j)
        pair(j - 1)

    grad(jnp.int32(0))
    loop(4, grad_and_pair, 1)
    pair(jnp.int32(3))

    tok_wait(2)
    gains = gain[:, cols(y)]
    e0 = lengths[0, 0]
    e1 = e0 + lengths[0, 1]
    e2 = e1 + lengths[0, 2]

    def ids(pos):
        return (
            (pos >= e0).astype(jnp.int32) + (pos >= e1).astype(jnp.int32) + (pos >= e2).astype(jnp.int32)
        )

    def attend(i):
        r = pl.ds(pl.multiple_of(i * TOK, TOK), TOK)
        scores = nt(qh[r], kh[...]) * (HEAD**-0.5)
        qid = ids(lax.broadcasted_iota(jnp.int32, (TOK, GROUP), 0) + i * TOK)
        kid = ids(lax.broadcasted_iota(jnp.int32, (TOK, GROUP), 1))
        scores = jnp.where(qid == kid, scores, -1e30)
        expo = jnp.exp(scores - jnp.max(scores, axis=-1, keepdims=True))
        probs = (expo / jnp.sum(expo, axis=-1, keepdims=True)).astype(BF16)
        view[r] = rms(mm(probs, vh[...]), gains).astype(BF16)

    loop(4, attend)

    def rz_copy(to):
        return remote(zs.at[to], zr.at[z], rz_s.at[to], rz_r.at[z], wide_1=to)

    def fold(j):
        p = part_of(j)
        for e in range(1, NX):
            remote(xs.at[x, p], xr.at[e, p], rx_s.at[e, p], rx_r.at[e, p], wide_0=x).wait_recv()
        total = xs[x, p].astype(F32)
        for e in range(1, NX):
            total = total + xr[e, p].astype(F32)
        for t in range(4):
            zs[p * 4 + t] = total[:, t * 8 : (t + 1) * 8].astype(BF16)
        for t in range(4):

            @pl.when(p * 4 + t != z)
            def _():
                rz_copy(p * 4 + t).start()

    loop(4, fold)
    zr[z] = zs[z]
    gather_sent(wbuf, wz_s, wz_r, wx_s, wx_r, wc_s, wc_r)

    def summed(d, total):
        frm = lax.rem(z + NZ - d, NZ)
        remote(zs.at[frm], zr.at[frm], rz_s.at[frm], rz_r.at[frm], wide_1=frm).wait_recv()
        return total + zr[frm].astype(F32)

    total = lax.fori_loop(1, NZ, summed, zr[z].astype(F32))
    mbuf[chip, c] = (momentum_decay * mhalf[...] + total * TOKENS**-0.5).astype(BF16)
    gather(mbuf, mz_s, mz_r, mx_s, mx_r, mc_s, mc_r)

    def squares(i, sums):
        b = pl.ds(pl.multiple_of(i * NZ, NZ), NZ)
        return tuple(
            s + jnp.sum(jnp.square(mbuf[b, 0, t].astype(F32)) + jnp.square(mbuf[b, 1, t].astype(F32)), axis=0)
            for t, s in enumerate(sums)
        )

    blank = jnp.zeros((8, HALF), F32)
    sums = lax.fori_loop(0, NX, squares, (blank, blank, blank))
    steps = tuple(
        step_size * lax.rsqrt(jnp.sum(jnp.sum(s, axis=1, keepdims=True), axis=0, keepdims=True) / HEAD**2 + epsilon)
        for s in sums
    )

    def moved_rows(w0, w1, m0, m1, step):
        v0 = w0 - m0 * step
        v1 = w1 - m1 * step
        before = jnp.sum(w0 * w0 + w1 * w1, axis=-1, keepdims=True) + epsilon
        after = jnp.sum(v0 * v0 + v1 * v1, axis=-1, keepdims=True) + epsilon
        ratio = jnp.sqrt(before) / jnp.sqrt(after)
        return v0 * ratio, v1 * ratio

    def renew(i):
        r = pl.ds(pl.multiple_of(i * TOK, TOK), TOK)
        b = pl.ds(pl.multiple_of(i * NZ, NZ), NZ)
        for t in range(3):
            parts = moved_rows(
                *(
                    buf[b, h, t].astype(F32).reshape(TOK, HALF)
                    for buf in (wbuf, mbuf)
                    for h in range(2)
                ),
                steps[t],
            )
            for h in range(2):
                n2[t, r, h * HALF : (h + 1) * HALF] = parts[h].astype(BF16)

    loop(4, renew)
    for d in range(1, NY):
        tok_copy(2, d).wait_send()

    def turn(i):
        return 1 + 2 * i - 3 * lax.div(i, 2)

    def o_copy(i):
        to = lax.rem(y + turn(i), NY)
        return remote(oblk.at[i], out.at[:, cols(y)], o_s.at[i], o_r.at[i], narrow=to)

    def apply(i):
        r = rows(lax.rem(y + turn(i), NY))
        qb = qh[r]
        pre_gate = mm(qb, n2[0])
        pre_up = mm(qb, n2[1])
        hidden = (pre_gate * jax.nn.sigmoid(pre_gate) * pre_up).astype(BF16)
        fast = rms(mm(hidden, n2[2]), gains).astype(BF16)
        oblk[i] = (view[r].astype(F32) + fast.astype(F32)).astype(BF16)

        @pl.when(i < NY - 1)
        def _():
            o_copy(i).start()

    loop(NY, apply)
    keep = pltpu.make_async_copy(oblk.at[NY - 1], out.at[:, cols(y)], o_own)
    keep.start()

    for t in range(3):
        m0, m1 = mbuf[chip, 0, t].astype(F32), mbuf[chip, 1, t].astype(F32)
        parts = moved_rows(wbuf[chip, 0, t].astype(F32), wbuf[chip, 1, t].astype(F32), m0, m1, steps[t])
        whole = jnp.concatenate(parts, axis=1)
        newv[t] = jnp.where(first, whole[:4], whole[4:]).astype(BF16)
        whole = jnp.concatenate([m0, m1], axis=1)
        momv[t] = jnp.where(first, whole[:4], whole[4:])
    done = [
        pltpu.make_async_copy(newv, new_out, small_sem.at[0]),
        pltpu.make_async_copy(momv, mom_out, small_sem.at[1]),
    ]
    for copy in done:
        copy.start()

    swap.wait_send()
    for t in range(2):
        for d in range(1, NY):
            tok_copy(t, d).wait_send()
    for b in range(NX):
        g_copy(b).wait_send()
    for j in range(4):
        for e in range(1, NX):
            rx_copy(jnp.int32(j), e).wait_send()

    def z_sent(d):
        rz_copy(lax.rem(z + d, NZ)).wait_send()

    loop(NZ, z_sent, 1)
    gather_sent(mbuf, mz_s, mz_r, mx_s, mx_r, mc_s, mc_r)
    for i, d in enumerate((1, 3, 2)):
        frm = lax.rem(y + NY - d, NY)
        remote(oblk.at[i], out.at[:, cols(frm)], o_s.at[i], o_r.at[i], narrow=frm).wait()
    keep.wait()
    for copy in done:
        copy.wait()


def deliver(out_in, new_in, mom_in, out, ng, nu, nd, og, ou, od, outv, newv, momv, sems):
    quarter = TOK // 4
    parts = [pl.ds(i * quarter, quarter) for i in range(4)]
    get = [pltpu.make_async_copy(new_in, newv, sems.at[0]), pltpu.make_async_copy(mom_in, momv, sems.at[1])]
    get += [pltpu.make_async_copy(out_in.at[p], outv.at[p], sems.at[2 + i]) for i, p in enumerate(parts)]
    put = [
        [pltpu.make_async_copy(newv.at[t], o.at[0], sems.at[6 + t]) for t, o in enumerate((ng, nu, nd))],
        [pltpu.make_async_copy(momv.at[t], o.at[0], sems.at[9 + t]) for t, o in enumerate((og, ou, od))],
        *([pltpu.make_async_copy(outv.at[p], out.at[p], sems.at[12 + i])] for i, p in enumerate(parts)),
    ]
    for copy in get:
        copy.start()
    for copy, then in zip(get, put):
        copy.wait()
        for other in then:
            other.start()
    for then in put:
        for other in then:
            other.wait()


def per_device(queries, keys, values, view_lengths, gain, *weights):
    hbm = pl.BlockSpec(memory_space=pltpu.HBM)
    dma = pltpu.SemaphoreType.DMA
    sq = (HEAD, HEAD)
    row = (4, HEAD)
    gather_sems = [dma((NZ,)), dma((NZ,)), dma((NX, NZ)), dma((NX, NZ)), dma, dma]
    parts = pl.pallas_call(
        kernel,
        out_shape=(
            jax.ShapeDtypeStruct(queries.shape, BF16),
            jax.ShapeDtypeStruct((3, *row), BF16),
            jax.ShapeDtypeStruct((3, *row), F32),
        ),
        in_specs=[hbm] * 11,
        out_specs=(hbm,) * 3,
        scratch_shapes=[
            pltpu.SMEM(view_lengths.shape, jnp.int32),
            pltpu.VMEM((1, gain.shape[0]), F32),
            pltpu.VMEM((3, *row), BF16),
            pltpu.VMEM((3, *row), BF16),
            pltpu.VMEM((3, *row), F32),
            dma((8,)),
            *[pltpu.VMEM(sq, BF16)] * 8,
            pltpu.VMEM((6, *row), F32),
            pltpu.VMEM((6, *row), F32),
            pltpu.VMEM((3, 8, HALF), F32),
            pltpu.VMEM((CHIPS, 2, 3, 8, HALF), BF16),
            pltpu.VMEM((3, HEAD, HEAD), BF16),
            pltpu.VMEM((4, NX, 3, 32, HALF), F32),
            pltpu.VMEM((4, NX, 3, 32, HALF), BF16),
            pltpu.VMEM((4, NX, 3, 32, HALF), BF16),
            pltpu.VMEM((NX, 4, 3, 32, HALF), BF16),
            pltpu.VMEM((NX, 4, 3, 32, HALF), BF16),
            pltpu.VMEM((NZ, 3, 8, HALF), BF16),
            pltpu.VMEM((NZ, 3, 8, HALF), BF16),
            pltpu.VMEM((CHIPS, 2, 3, 8, HALF), BF16),
            pltpu.VMEM((3, HEAD, HEAD), BF16),
            pltpu.VMEM(sq, BF16),
            pltpu.VMEM((NY, TOK, HEAD), BF16),
            dma((3, NY)), dma((3, NY)), dma((3,)), dma((2,)),
            *gather_sems,
            *gather_sems,
            dma((NX,)), dma((NX,)), dma((NX, 4)), dma((NX, 4)), dma((NZ,)), dma((NZ,)),
            dma((NY,)), dma((NY,)), dma,
        ],
        compiler_params=pltpu.CompilerParams(
            collective_id=0, has_side_effects=True, vmem_limit_bytes=67_043_328
        ),
    )(queries, keys, values, view_lengths, gain.reshape(1, -1), *weights)
    return pl.pallas_call(
        deliver,
        out_shape=(
            jax.ShapeDtypeStruct(queries.shape, BF16),
            *[jax.ShapeDtypeStruct((1, *row), BF16)] * 3,
            *[jax.ShapeDtypeStruct((1, *row), F32)] * 3,
        ),
        in_specs=[hbm] * 3,
        out_specs=(hbm,) * 7,
        scratch_shapes=[
            pltpu.VMEM(queries.shape, BF16),
            pltpu.VMEM((3, *row), BF16),
            pltpu.VMEM((3, *row), F32),
            dma((16,)),
        ],
        compiler_params=pltpu.CompilerParams(vmem_limit_bytes=67_043_328),
    )(*parts)


def solution(mesh):
    split = Mesh(
        mesh.devices.reshape(NX, NZ, 2, mesh.shape["narrow"]),
        ("wide_0", "wide_1", "wide_2", "narrow"),
    )
    rows = P("narrow", WIDE, None)
    return jax.shard_map(
        per_device,
        mesh=split,
        in_specs=(*[P(WIDE_NARROW, None)] * 3, P(WIDE, None), P(), *[rows] * 6),
        out_specs=(P(WIDE_NARROW, None), *[rows] * 6),
        check_vma=False,
    )
```

```python
import functools

import jax
import jax.numpy as jnp
from jax import lax
from jax.experimental import pallas as pl
from jax.experimental.pallas import tpu as pltpu
from jax.sharding import Mesh
from jax.sharding import PartitionSpec as P

WIDE = ("wide_0", "wide_1", "wide_2")
WIDE_NARROW = ("wide_0", "wide_1", "wide_2", "narrow")
MESH = pl.DeviceIdType.MESH

momentum_decay = 0.9
step_size = 0.02
epsilon = 1e-06

NX, NZ, NY = 4, 16, 4
NEAR = 4
RELAY_HOPS = (1, 2, 3, 4)
OWN_RUN = (0, 1)
NEAR_RUNS = ((1, 4), (12, 4))
FAR_RUNS = ((5, 2), (10, 2), (7, 3))
RUNS = (OWN_RUN, *NEAR_RUNS, *FAR_RUNS)
HEAD = 512
HALF = 256
GROUP = 512
TOK = 128
TOKENS = 65536
F32 = jnp.float32
BF16 = jnp.bfloat16


def nt(a, b):
    return lax.dot_general(a, b, (((1,), (1,)), ((), ())), preferred_element_type=F32)


def mm(a, b):
    return jnp.dot(a, b, preferred_element_type=F32)


def rms(field, gains):
    return field * lax.rsqrt(jnp.mean(field * field, axis=-1, keepdims=True) + epsilon) * gains


def remote(src, dst, send, recv, **where):
    return pltpu.make_async_remote_copy(
        src_ref=src, dst_ref=dst, send_sem=send, recv_sem=recv, device_id=where, device_id_type=MESH
    )


def loop(n, body, start=0):
    def step(i, carry):
        body(i)
        return carry

    lax.fori_loop(start, n, step, 0)


def kernel(
    q_in, k_in, v_in, lengths_in, gain_in, wg, wu, wd, mg, mu, md,
    out, new_out, mom_out,
    lengths, gain, wrow, newv, momv, small_sem,
    qh, kh, vh, kt, ht, hid, dg, du, ex, exr, mhalf, wbuf, w2, own, gsend, grecv,
    xs, xr, zs, zr, mbuf, n2, view, oblk,
    tok_send, tok_recv, tok_own, ex_sem, wz_s, wz_r, wx_s, wx_r, wc_s, wc_r,
    mz_s, mz_r, mx_s, mx_r, mc_s, mc_r, gs_s, gs_r, rx_s, rx_r, rz_s, rz_r, o_s, o_r, o_own,
):
    x = lax.axis_index("wide_0")
    z = lax.axis_index("wide_1")
    c = lax.axis_index("wide_2")
    y = lax.axis_index("narrow")
    other = 1 - c
    side = 1 + 2 * c

    small = [pltpu.make_async_copy(w.at[0], wrow.at[t], small_sem.at[t]) for t, w in enumerate((wg, wu, wd))]
    small += [pltpu.make_async_copy(m.at[0], ex.at[3 + t], small_sem.at[3 + t]) for t, m in enumerate((mg, mu, md))]
    small += [
        pltpu.make_async_copy(lengths_in, lengths, small_sem.at[6]),
        pltpu.make_async_copy(gain_in, gain, small_sem.at[7]),
    ]
    for copy in small:
        copy.start()

    barrier = pltpu.get_barrier_semaphore()
    pl.semaphore_signal(barrier, inc=1, device_id={"wide_2": other}, device_id_type=MESH)
    for d in range(1, NY):
        pl.semaphore_signal(
            barrier, inc=1, device_id={"narrow": lax.rem(y + d, NY)}, device_id_type=MESH
        )
    for d in range(1, NX):
        pl.semaphore_signal(
            barrier, inc=1, device_id={"wide_0": lax.rem(x + d, NX)}, device_id_type=MESH
        )

    def greet(d):
        pl.semaphore_signal(
            barrier, inc=1, device_id={"wide_1": lax.rem(z + d, NZ)}, device_id_type=MESH
        )

    for d in range(1, NEAR + 1):
        greet(d)
        greet(NZ - d)
    for copy in small:
        copy.wait()
    ex[:3] = wrow[...].astype(F32)
    pl.semaphore_wait(barrier, NY - 1 + NX - 1 + 2 * NEAR + 1)

    def cols(who):
        return pl.ds(pl.multiple_of(who * HEAD, HEAD), HEAD)

    def rows(who):
        return pl.ds(pl.multiple_of(who * TOK, TOK), TOK)

    trio = ((k_in, kh), (v_in, vh), (q_in, qh))

    def tok_copy(t, d):
        src, dst = trio[t]
        to = lax.rem(y + d, NY)
        return remote(
            src.at[:, cols(to)], dst.at[rows(y)], tok_send.at[t, d], tok_recv.at[t, d], narrow=to
        )

    def tok_wait(t):
        src, dst = trio[t]
        for d in range(1, NY):
            frm = lax.rem(y + NY - d, NY)
            remote(
                src.at[:, cols(y)], dst.at[rows(frm)], tok_send.at[t, d], tok_recv.at[t, d], narrow=frm
            ).wait_recv()
        tok_local(t).wait()

    def tok_local(t):
        src, dst = trio[t]
        return pltpu.make_async_copy(src.at[:, cols(y)], dst.at[rows(y)], tok_own.at[t])

    swap = remote(ex, exr, ex_sem.at[0], ex_sem.at[1], wide_2=other)
    swap.start()
    for t in range(3):
        for d in (side, 4 - side, 2):
            tok_copy(t, d).start()
        tok_local(t).start()

    def z_copy(buf, z_s, z_r, via, hop):
        d = (via + hop) % NZ
        return remote(
            buf.at[0, c, via], buf.at[0, c, d], z_s.at[d], z_r.at[d], wide_1=lax.rem(z + hop, NZ)
        )

    def x_copy(buf, x_s, x_r, e, k):
        a, n = RUNS[k]
        return remote(
            buf.at[0, c, pl.ds(a, n)], buf.at[e, c, pl.ds(a, n)], x_s.at[e, k], x_r.at[e, k],
            wide_0=lax.rem(x + e, NX),
        )

    def gather(buf, z_s, z_r, x_s, x_r, c_s, c_r, meanwhile=None):
        def across(e, k):
            a, n = RUNS[k]
            part = buf.at[e, c, pl.ds(a, n)]
            remote(part, part, c_s, c_r, wide_2=other).start()

        def forward(k, late=False):
            for e in (2, side, 4 - side) if late else (side, 4 - side, 2):
                x_copy(buf, x_s, x_r, e, k).start()
            across(0, k)

        def landed(d):
            z_copy(buf, z_s, z_r, d, 0).wait_recv()

        def arrived(k):
            for e in (1, 3, 2):
                x_copy(buf, x_s, x_r, e, k).wait_recv()
                across(e, k)

        for d in range(NEAR, 0, -1):
            z_copy(buf, z_s, z_r, 0, d).start()
            z_copy(buf, z_s, z_r, 0, NZ - d).start()
        forward(0)
        landed(NEAR)
        for hop in RELAY_HOPS:
            z_copy(buf, z_s, z_r, NEAR, hop).start()
        landed(NZ - NEAR)
        for hop in RELAY_HOPS:
            if NEAR + hop < NZ // 2:
                z_copy(buf, z_s, z_r, NZ - NEAR, NZ - hop).start()
        for k, (a, n) in enumerate(RUNS):
            if k == 0:
                continue
            if k == 1 + len(NEAR_RUNS):
                arrived(0)
            for d in range(a, a + n):
                if d not in (NEAR, NZ - NEAR):
                    landed(d)
            forward(k, k > len(NEAR_RUNS))
        if meanwhile is not None:
            meanwhile()
        for k in range(1, len(RUNS)):
            arrived(k)
        part = buf.at[:, other]
        remote(part, part, c_s, c_r, wide_2=other).wait_recv()

    def gather_sent(buf, z_s, z_r, x_s, x_r, c_s, c_r):
        for d in range(1, NZ):
            z_copy(buf, z_s, z_r, 0, d).wait_send()
        for k in range(len(RUNS)):
            for e in range(1, NX):
                x_copy(buf, x_s, x_r, e, k).wait_send()
        part = buf.at[:, c]
        remote(part, part, c_s, c_r, wide_2=other).wait_send()

    def tall(buf, i, h, t):
        e = lax.rem(x + NX - i, NX)
        return jnp.concatenate(
            [buf[e, h, lax.rem(z + NZ - b, NZ), t].astype(F32) for b in range(NZ)], axis=0
        )

    swap.wait_recv()
    mine, theirs = ex[...], exr[...]
    first = c == 0
    rows8 = jnp.concatenate(
        [jnp.where(first, mine, theirs), jnp.where(first, theirs, mine)], axis=1
    )
    half = jnp.where(first, rows8[:, :, :HALF], rows8[:, :, HALF:])
    wbuf[0, c, 0] = half[:3].astype(BF16)
    mhalf[...] = half[3:]

    def turn_keys():
        tok_wait(0)
        kt[...] = kh[...].T

    gather(wbuf, wz_s, wz_r, wx_s, wx_r, wc_s, wc_r, turn_keys)

    def square(i):
        r = pl.ds(pl.multiple_of(i * TOK, TOK), TOK)
        for t in range(3):
            for h in range(2):
                w2[t, r, h * HALF : (h + 1) * HALF] = tall(wbuf, i, h, t).astype(BF16)

    loop(4, square)
    tok_wait(1)


    def back(i):
        r = pl.ds(pl.multiple_of(i * TOK, TOK), TOK)
        kb = kh[r]
        pre_gate = mm(kb, w2[0])
        pre_up = mm(kb, w2[1])
        d_hidden = -nt(vh[r], w2[2])
        sig = jax.nn.sigmoid(pre_gate)
        activ = pre_gate * sig
        hid[r] = (activ * pre_up).astype(BF16)
        dg[r] = (d_hidden * pre_up * (sig * (1.0 + pre_gate * (1.0 - sig)))).astype(BF16)
        du[r] = (d_hidden * activ).astype(BF16)

    loop(4, back)
    ht[...] = hid[...].T

    def g_copy(b):
        return remote(gsend.at[b], grecv.at[b], gs_s.at[b], gs_r.at[b], wide_2=other)

    def part_of(j):
        return lax.rem(lax.div(z, 4) + 2 + j + lax.div(j * (j - 1), 2), 4)

    def grad(j):
        p = part_of(j)
        quarter = [pl.ds(pl.multiple_of(b * TOK + p * 32, 32), 32) for b in range(NX)]
        kb = jnp.concatenate([kt[r] for r in quarter], axis=0)
        hb = jnp.concatenate([ht[r] for r in quarter], axis=0)
        for t, g in enumerate((mm(kb, dg[...]), mm(kb, du[...]), -mm(hb, vh[...]))):
            keep = jnp.where(first, g[:, :HALF], g[:, HALF:])
            give = jnp.where(first, g[:, HALF:], g[:, :HALF]).astype(BF16)
            for b in range(NX):
                own[p, b, t] = keep[b * 32 : (b + 1) * 32]
                gsend[p, b, t] = give[b * 32 : (b + 1) * 32]
        g_copy(p).start()

    def rx_copy(j, e):
        to = lax.rem(x + e, NX)
        p = part_of(j)
        return remote(xs.at[to, p], xr.at[e, p], rx_s.at[e, p], rx_r.at[e, p], wide_0=to)

    def pair(j):
        p = part_of(j)
        g_copy(p).wait_recv()
        for b in range(NX):
            for t in range(3):
                xs[b, p, t] = (own[p, b, t] + grecv[p, b, t].astype(F32)).astype(BF16)
        for e in (side, 4 - side, 2):
            rx_copy(j, e).start()

    def grad_and_pair(j):
        grad(j)
        pair(j - 1)

    grad(jnp.int32(0))
    loop(4, grad_and_pair, 1)
    pair(jnp.int32(3))

    tok_wait(2)
    gains = gain[:, cols(y)]
    e0 = lengths[0, 0]
    e1 = e0 + lengths[0, 1]
    e2 = e1 + lengths[0, 2]

    def ids(pos):
        return (
            (pos >= e0).astype(jnp.int32) + (pos >= e1).astype(jnp.int32) + (pos >= e2).astype(jnp.int32)
        )

    def attend(i):
        r = pl.ds(pl.multiple_of(i * TOK, TOK), TOK)
        scores = nt(qh[r], kh[...]) * (HEAD**-0.5)
        qid = ids(lax.broadcasted_iota(jnp.int32, (TOK, GROUP), 0) + i * TOK)
        kid = ids(lax.broadcasted_iota(jnp.int32, (TOK, GROUP), 1))
        scores = jnp.where(qid == kid, scores, -1e30)
        expo = jnp.exp(scores - jnp.max(scores, axis=-1, keepdims=True))
        probs = (expo / jnp.sum(expo, axis=-1, keepdims=True)).astype(BF16)
        view[r] = rms(mm(probs, vh[...]), gains).astype(BF16)

    loop(4, attend)

    def rz_copy(to):
        return remote(zs.at[to], zr.at[z], rz_s.at[to], rz_r.at[z], wide_1=to)

    def fold(j):
        p = part_of(j)
        for e in range(1, NX):
            remote(xs.at[x, p], xr.at[e, p], rx_s.at[e, p], rx_r.at[e, p], wide_0=x).wait_recv()
        total = xs[x, p].astype(F32)
        for e in range(1, NX):
            total = total + xr[e, p].astype(F32)
        for t in range(4):
            zs[p * 4 + t] = total[:, t * 8 : (t + 1) * 8].astype(BF16)
        for t in range(4):

            @pl.when(p * 4 + t != z)
            def _():
                rz_copy(p * 4 + t).start()

    loop(4, fold)
    zr[z] = zs[z]
    gather_sent(wbuf, wz_s, wz_r, wx_s, wx_r, wc_s, wc_r)

    def summed(d, total):
        frm = lax.rem(z + NZ - d, NZ)
        remote(zs.at[frm], zr.at[frm], rz_s.at[frm], rz_r.at[frm], wide_1=frm).wait_recv()
        return total + zr[frm].astype(F32)

    total = lax.fori_loop(1, NZ, summed, zr[z].astype(F32))
    mbuf[0, c, 0] = (momentum_decay * mhalf[...] + total * TOKENS**-0.5).astype(BF16)
    gather(mbuf, mz_s, mz_r, mx_s, mx_r, mc_s, mc_r)

    def squares(i, sums):
        return tuple(
            s + jnp.sum(jnp.square(mbuf[i, 0, :, t].astype(F32)) + jnp.square(mbuf[i, 1, :, t].astype(F32)), axis=0)
            for t, s in enumerate(sums)
        )

    blank = jnp.zeros((8, HALF), F32)
    sums = lax.fori_loop(0, NX, squares, (blank, blank, blank))
    steps = tuple(
        step_size * lax.rsqrt(jnp.sum(jnp.sum(s, axis=1, keepdims=True), axis=0, keepdims=True) / HEAD**2 + epsilon)
        for s in sums
    )

    def moved_rows(w0, w1, m0, m1, step):
        v0 = w0 - m0 * step
        v1 = w1 - m1 * step
        before = jnp.sum(w0 * w0 + w1 * w1, axis=-1, keepdims=True) + epsilon
        after = jnp.sum(v0 * v0 + v1 * v1, axis=-1, keepdims=True) + epsilon
        ratio = jnp.sqrt(before) / jnp.sqrt(after)
        return v0 * ratio, v1 * ratio

    def renew(i):
        r = pl.ds(pl.multiple_of(i * TOK, TOK), TOK)
        for t in range(3):
            parts = moved_rows(*(tall(buf, i, h, t) for buf in (wbuf, mbuf) for h in range(2)), steps[t])
            for h in range(2):
                n2[t, r, h * HALF : (h + 1) * HALF] = parts[h].astype(BF16)

    loop(4, renew)
    for d in range(1, NY):
        tok_copy(2, d).wait_send()

    def turn(i):
        late = lax.div(i, 2)
        return (1 - late) * lax.rem(1 + 2 * i + 2 * c, 4) + late * (2 * i - 2)

    def o_copy(i):
        to = lax.rem(y + turn(i), NY)
        return remote(oblk.at[i], out.at[:, cols(y)], o_s.at[i], o_r.at[i], narrow=to)

    def apply(i):
        r = rows(lax.rem(y + turn(i), NY))
        qb = qh[r]
        pre_gate = mm(qb, n2[0])
        pre_up = mm(qb, n2[1])
        hidden = (pre_gate * jax.nn.sigmoid(pre_gate) * pre_up).astype(BF16)
        fast = rms(mm(hidden, n2[2]), gains).astype(BF16)
        oblk[i] = (view[r].astype(F32) + fast.astype(F32)).astype(BF16)

        @pl.when(i < NY - 1)
        def _():
            o_copy(i).start()

    loop(NY, apply)
    keep = pltpu.make_async_copy(oblk.at[NY - 1], out.at[:, cols(y)], o_own)
    keep.start()

    for t in range(3):
        m0, m1 = mbuf[0, 0, 0, t].astype(F32), mbuf[0, 1, 0, t].astype(F32)
        parts = moved_rows(wbuf[0, 0, 0, t].astype(F32), wbuf[0, 1, 0, t].astype(F32), m0, m1, steps[t])
        whole = jnp.concatenate(parts, axis=1)
        newv[t] = jnp.where(first, whole[:4], whole[4:]).astype(BF16)
        whole = jnp.concatenate([m0, m1], axis=1)
        momv[t] = jnp.where(first, whole[:4], whole[4:])
    done = [
        pltpu.make_async_copy(newv, new_out, small_sem.at[0]),
        pltpu.make_async_copy(momv, mom_out, small_sem.at[1]),
    ]
    for copy in done:
        copy.start()

    swap.wait_send()
    for t in range(2):
        for d in range(1, NY):
            tok_copy(t, d).wait_send()
    for b in range(NX):
        g_copy(b).wait_send()
    for j in range(4):
        for e in range(1, NX):
            rx_copy(jnp.int32(j), e).wait_send()

    def z_sent(d):
        rz_copy(lax.rem(z + d, NZ)).wait_send()

    loop(NZ, z_sent, 1)
    gather_sent(mbuf, mz_s, mz_r, mx_s, mx_r, mc_s, mc_r)
    for i in range(NY - 1):
        frm = lax.rem(y + NY - turn(i), NY)
        remote(oblk.at[i], out.at[:, cols(frm)], o_s.at[i], o_r.at[i], narrow=frm).wait()
    keep.wait()
    for copy in done:
        copy.wait()


def deliver(out_in, new_in, mom_in, out, ng, nu, nd, og, ou, od, outv, newv, momv, sems):
    quarter = TOK // 4
    parts = [pl.ds(i * quarter, quarter) for i in range(4)]
    get = [pltpu.make_async_copy(new_in, newv, sems.at[0]), pltpu.make_async_copy(mom_in, momv, sems.at[1])]
    get += [pltpu.make_async_copy(out_in.at[p], outv.at[p], sems.at[2 + i]) for i, p in enumerate(parts)]
    put = [
        [pltpu.make_async_copy(newv.at[t], o.at[0], sems.at[6 + t]) for t, o in enumerate((ng, nu, nd))],
        [pltpu.make_async_copy(momv.at[t], o.at[0], sems.at[9 + t]) for t, o in enumerate((og, ou, od))],
        *([pltpu.make_async_copy(outv.at[p], out.at[p], sems.at[12 + i])] for i, p in enumerate(parts)),
    ]
    for copy in get:
        copy.start()
    for copy, then in zip(get, put):
        copy.wait()
        for other in then:
            other.start()
    for then in put:
        for other in then:
            other.wait()


def per_device(queries, keys, values, view_lengths, gain, *weights):
    hbm = pl.BlockSpec(memory_space=pltpu.HBM)
    dma = pltpu.SemaphoreType.DMA
    sq = (HEAD, HEAD)
    row = (4, HEAD)
    gather_sems = [dma((NZ,)), dma((NZ,)), dma((NX, len(RUNS))), dma((NX, len(RUNS))), dma, dma]
    parts = pl.pallas_call(
        kernel,
        out_shape=(
            jax.ShapeDtypeStruct(queries.shape, BF16),
            jax.ShapeDtypeStruct((3, *row), BF16),
            jax.ShapeDtypeStruct((3, *row), F32),
        ),
        in_specs=[hbm] * 11,
        out_specs=(hbm,) * 3,
        scratch_shapes=[
            pltpu.SMEM(view_lengths.shape, jnp.int32),
            pltpu.VMEM((1, gain.shape[0]), F32),
            pltpu.VMEM((3, *row), BF16),
            pltpu.VMEM((3, *row), BF16),
            pltpu.VMEM((3, *row), F32),
            dma((8,)),
            *[pltpu.VMEM(sq, BF16)] * 8,
            pltpu.VMEM((6, *row), F32),
            pltpu.VMEM((6, *row), F32),
            pltpu.VMEM((3, 8, HALF), F32),
            pltpu.VMEM((NX, 2, NZ, 3, 8, HALF), BF16),
            pltpu.VMEM((3, HEAD, HEAD), BF16),
            pltpu.VMEM((4, NX, 3, 32, HALF), F32),
            pltpu.VMEM((4, NX, 3, 32, HALF), BF16),
            pltpu.VMEM((4, NX, 3, 32, HALF), BF16),
            pltpu.VMEM((NX, 4, 3, 32, HALF), BF16),
            pltpu.VMEM((NX, 4, 3, 32, HALF), BF16),
            pltpu.VMEM((NZ, 3, 8, HALF), BF16),
            pltpu.VMEM((NZ, 3, 8, HALF), BF16),
            pltpu.VMEM((NX, 2, NZ, 3, 8, HALF), BF16),
            pltpu.VMEM((3, HEAD, HEAD), BF16),
            pltpu.VMEM(sq, BF16),
            pltpu.VMEM((NY, TOK, HEAD), BF16),
            dma((3, NY)), dma((3, NY)), dma((3,)), dma((2,)),
            *gather_sems,
            *gather_sems,
            dma((NX,)), dma((NX,)), dma((NX, 4)), dma((NX, 4)), dma((NZ,)), dma((NZ,)),
            dma((NY,)), dma((NY,)), dma,
        ],
        compiler_params=pltpu.CompilerParams(
            collective_id=0, has_side_effects=True, vmem_limit_bytes=67_043_328
        ),
    )(queries, keys, values, view_lengths, gain.reshape(1, -1), *weights)
    return pl.pallas_call(
        deliver,
        out_shape=(
            jax.ShapeDtypeStruct(queries.shape, BF16),
            *[jax.ShapeDtypeStruct((1, *row), BF16)] * 3,
            *[jax.ShapeDtypeStruct((1, *row), F32)] * 3,
        ),
        in_specs=[hbm] * 3,
        out_specs=(hbm,) * 7,
        scratch_shapes=[
            pltpu.VMEM(queries.shape, BF16),
            pltpu.VMEM((3, *row), BF16),
            pltpu.VMEM((3, *row), F32),
            dma((16,)),
        ],
        compiler_params=pltpu.CompilerParams(vmem_limit_bytes=67_043_328),
    )(*parts)


def solution(mesh):
    split = Mesh(
        mesh.devices.reshape(NX, NZ, 2, mesh.shape["narrow"]),
        ("wide_0", "wide_1", "wide_2", "narrow"),
    )
    rows = P("narrow", WIDE, None)
    return jax.shard_map(
        per_device,
        mesh=split,
        in_specs=(*[P(WIDE_NARROW, None)] * 3, P(WIDE, None), P(), *[rows] * 6),
        out_specs=(P(WIDE_NARROW, None), *[rows] * 6),
        check_vma=False,
    )
```

```python
import functools

import jax
import jax.numpy as jnp
from jax import lax
from jax.experimental import pallas as pl
from jax.experimental.pallas import tpu as pltpu
from jax.sharding import Mesh
from jax.sharding import PartitionSpec as P

WIDE = ("wide_0", "wide_1", "wide_2")
WIDE_NARROW = ("wide_0", "wide_1", "wide_2", "narrow")
MESH = pl.DeviceIdType.MESH

momentum_decay = 0.9
step_size = 0.02
epsilon = 1e-06

NX, NZ, NY = 4, 16, 4
NEAR = 3
STAGES = tuple(range(NEAR, NZ // 2, NEAR))
LAST = STAGES[-1] + 1
RUNS = (
    (0, 1),
    *((a, NEAR) for p in STAGES for a in (p - NEAR + 1, NZ - p)),
    (LAST, NZ + 1 - 2 * LAST),
)
HEAD = 512
HALF = 256
GROUP = 512
TOK = 128
TOKENS = 65536
F32 = jnp.float32
BF16 = jnp.bfloat16


def nt(a, b):
    return lax.dot_general(a, b, (((1,), (1,)), ((), ())), preferred_element_type=F32)


def mm(a, b):
    return jnp.dot(a, b, preferred_element_type=F32)


def rms(field, gains):
    return field * lax.rsqrt(jnp.mean(field * field, axis=-1, keepdims=True) + epsilon) * gains


def remote(src, dst, send, recv, **where):
    return pltpu.make_async_remote_copy(
        src_ref=src, dst_ref=dst, send_sem=send, recv_sem=recv, device_id=where, device_id_type=MESH
    )


def loop(n, body, start=0):
    def step(i, carry):
        body(i)
        return carry

    lax.fori_loop(start, n, step, 0)


def kernel(
    q_in, k_in, v_in, lengths_in, gain_in, wg, wu, wd, mg, mu, md,
    out, new_out, mom_out,
    lengths, gain, wrow, newv, momv, small_sem,
    qh, kh, vh, kt, ht, hid, dg, du, ex, exr, mhalf, wbuf, w2, own, gsend, grecv,
    xs, xr, zs, zr, mbuf, n2, view, oblk,
    tok_send, tok_recv, tok_own, ex_sem, wz_s, wz_r, wx_s, wx_r, wc_s, wc_r,
    mz_s, mz_r, mx_s, mx_r, mc_s, mc_r, gs_s, gs_r, rx_s, rx_r, rz_s, rz_r, o_s, o_r, o_own,
):
    x = lax.axis_index("wide_0")
    z = lax.axis_index("wide_1")
    c = lax.axis_index("wide_2")
    y = lax.axis_index("narrow")
    other = 1 - c
    side = 1 + 2 * c

    small = [pltpu.make_async_copy(w.at[0], wrow.at[t], small_sem.at[t]) for t, w in enumerate((wg, wu, wd))]
    small += [pltpu.make_async_copy(m.at[0], ex.at[3 + t], small_sem.at[3 + t]) for t, m in enumerate((mg, mu, md))]
    small += [
        pltpu.make_async_copy(lengths_in, lengths, small_sem.at[6]),
        pltpu.make_async_copy(gain_in, gain, small_sem.at[7]),
    ]
    for copy in small:
        copy.start()

    barrier = pltpu.get_barrier_semaphore()
    pl.semaphore_signal(barrier, inc=1, device_id={"wide_2": other}, device_id_type=MESH)
    for d in range(1, NY):
        pl.semaphore_signal(
            barrier, inc=1, device_id={"narrow": lax.rem(y + d, NY)}, device_id_type=MESH
        )
    for d in range(1, NX):
        pl.semaphore_signal(
            barrier, inc=1, device_id={"wide_0": lax.rem(x + d, NX)}, device_id_type=MESH
        )

    def greet(d):
        pl.semaphore_signal(
            barrier, inc=1, device_id={"wide_1": lax.rem(z + d, NZ)}, device_id_type=MESH
        )

    for d in range(1, NEAR + 1):
        greet(d)
        greet(NZ - d)
    for copy in small:
        copy.wait()
    ex[:3] = wrow[...].astype(F32)
    pl.semaphore_wait(barrier, NY - 1 + NX - 1 + 2 * NEAR + 1)

    def cols(who):
        return pl.ds(pl.multiple_of(who * HEAD, HEAD), HEAD)

    def rows(who):
        return pl.ds(pl.multiple_of(who * TOK, TOK), TOK)

    trio = ((k_in, kh), (v_in, vh), (q_in, qh))

    def tok_copy(t, d):
        src, dst = trio[t]
        to = lax.rem(y + d, NY)
        return remote(
            src.at[:, cols(to)], dst.at[rows(y)], tok_send.at[t, d], tok_recv.at[t, d], narrow=to
        )

    def tok_wait(t):
        src, dst = trio[t]
        for d in range(1, NY):
            frm = lax.rem(y + NY - d, NY)
            remote(
                src.at[:, cols(y)], dst.at[rows(frm)], tok_send.at[t, d], tok_recv.at[t, d], narrow=frm
            ).wait_recv()
        tok_local(t).wait()

    def tok_local(t):
        src, dst = trio[t]
        return pltpu.make_async_copy(src.at[:, cols(y)], dst.at[rows(y)], tok_own.at[t])

    swap = remote(ex, exr, ex_sem.at[0], ex_sem.at[1], wide_2=other)
    swap.start()
    for t in range(3):
        for d in (side, 4 - side, 2):
            tok_copy(t, d).start()
        tok_local(t).start()

    def z_copy(buf, z_s, z_r, via, hop):
        d = (via + hop) % NZ
        return remote(
            buf.at[0, c, via], buf.at[0, c, d], z_s.at[d], z_r.at[d], wide_1=lax.rem(z + hop, NZ)
        )

    def x_copy(buf, x_s, x_r, e, k):
        a, n = RUNS[k]
        return remote(
            buf.at[0, c, pl.ds(a, n)], buf.at[e, c, pl.ds(a, n)], x_s.at[e, k], x_r.at[e, k],
            wide_0=lax.rem(x + e, NX),
        )

    def gather(buf, z_s, z_r, x_s, x_r, c_s, c_r, meanwhile=None):
        def across(e, k):
            a, n = RUNS[k]
            part = buf.at[e, c, pl.ds(a, n)]
            remote(part, part, c_s, c_r, wide_2=other).start()

        def forward(k, late=False):
            for e in (2, side, 4 - side) if late else (side, 4 - side, 2):
                x_copy(buf, x_s, x_r, e, k).start()
            across(0, k)

        def landed(d):
            z_copy(buf, z_s, z_r, d, 0).wait_recv()

        def arrived(k):
            for e in (1, 3, 2):
                x_copy(buf, x_s, x_r, e, k).wait_recv()
                across(e, k)

        def onward(p):
            hops = range(min(NEAR, NZ // 2 - p), 0, -1)
            for hop in hops:
                z_copy(buf, z_s, z_r, p, hop).start()

        def backward(p):
            for hop in range(min(NEAR, NZ // 2 - 1 - p), 0, -1):
                z_copy(buf, z_s, z_r, (NZ - p) % NZ, NZ - hop).start()

        onward(0)
        backward(0)
        forward(0)
        for k, p in enumerate(STAGES):
            landed(p)
            onward(p)
            landed(NZ - p)
            backward(p)
            for d in range(p - NEAR + 1, p):
                landed(d)
            forward(2 * k + 1)
            for d in range(NZ - p + 1, NZ - p + NEAR):
                landed(d)
            forward(2 * k + 2)
            if k == 0:
                arrived(0)
        for d in range(LAST, NZ + 1 - LAST):
            landed(d)
        forward(len(RUNS) - 1, True)
        if meanwhile is not None:
            meanwhile()
        for k in range(1, len(RUNS)):
            arrived(k)
        part = buf.at[:, other]
        remote(part, part, c_s, c_r, wide_2=other).wait_recv()

    def gather_sent(buf, z_s, z_r, x_s, x_r, c_s, c_r):
        for d in range(1, NZ):
            z_copy(buf, z_s, z_r, 0, d).wait_send()
        for k in range(len(RUNS)):
            for e in range(1, NX):
                x_copy(buf, x_s, x_r, e, k).wait_send()
        part = buf.at[:, c]
        remote(part, part, c_s, c_r, wide_2=other).wait_send()

    def tall(buf, i, h, t):
        e = lax.rem(x + NX - i, NX)
        return jnp.concatenate(
            [buf[e, h, lax.rem(z + NZ - b, NZ), t].astype(F32) for b in range(NZ)], axis=0
        )

    swap.wait_recv()
    mine, theirs = ex[...], exr[...]
    first = c == 0
    rows8 = jnp.concatenate(
        [jnp.where(first, mine, theirs), jnp.where(first, theirs, mine)], axis=1
    )
    half = jnp.where(first, rows8[:, :, :HALF], rows8[:, :, HALF:])
    wbuf[0, c, 0] = half[:3].astype(BF16)
    mhalf[...] = half[3:]

    def turn_keys():
        tok_wait(0)
        kt[...] = kh[...].T

    gather(wbuf, wz_s, wz_r, wx_s, wx_r, wc_s, wc_r, turn_keys)

    def square(i):
        r = pl.ds(pl.multiple_of(i * TOK, TOK), TOK)
        for t in range(3):
            for h in range(2):
                w2[t, r, h * HALF : (h + 1) * HALF] = tall(wbuf, i, h, t).astype(BF16)

    loop(4, square)
    tok_wait(1)


    def back(i):
        r = pl.ds(pl.multiple_of(i * TOK, TOK), TOK)
        kb = kh[r]
        pre_gate = mm(kb, w2[0])
        pre_up = mm(kb, w2[1])
        d_hidden = -nt(vh[r], w2[2])
        sig = jax.nn.sigmoid(pre_gate)
        activ = pre_gate * sig
        hid[r] = (activ * pre_up).astype(BF16)
        dg[r] = (d_hidden * pre_up * (sig * (1.0 + pre_gate * (1.0 - sig)))).astype(BF16)
        du[r] = (d_hidden * activ).astype(BF16)

    loop(4, back)
    ht[...] = hid[...].T

    def g_copy(b):
        return remote(gsend.at[b], grecv.at[b], gs_s.at[b], gs_r.at[b], wide_2=other)

    def part_of(j):
        return lax.rem(lax.div(z, 4) + 2 + j + lax.div(j * (j - 1), 2), 4)

    def grad(j):
        p = part_of(j)
        quarter = [pl.ds(pl.multiple_of(b * TOK + p * 32, 32), 32) for b in range(NX)]
        kb = jnp.concatenate([kt[r] for r in quarter], axis=0)
        hb = jnp.concatenate([ht[r] for r in quarter], axis=0)
        for t, g in enumerate((mm(kb, dg[...]), mm(kb, du[...]), -mm(hb, vh[...]))):
            keep = jnp.where(first, g[:, :HALF], g[:, HALF:])
            give = jnp.where(first, g[:, HALF:], g[:, :HALF]).astype(BF16)
            for b in range(NX):
                own[p, b, t] = keep[b * 32 : (b + 1) * 32]
                gsend[p, b, t] = give[b * 32 : (b + 1) * 32]
        g_copy(p).start()

    def rx_copy(j, e):
        to = lax.rem(x + e, NX)
        p = part_of(j)
        return remote(xs.at[to, p], xr.at[e, p], rx_s.at[e, p], rx_r.at[e, p], wide_0=to)

    def pair(j):
        p = part_of(j)
        g_copy(p).wait_recv()
        for b in range(NX):
            for t in range(3):
                xs[b, p, t] = (own[p, b, t] + grecv[p, b, t].astype(F32)).astype(BF16)
        for e in (side, 4 - side, 2):
            rx_copy(j, e).start()

    def grad_and_pair(j):
        grad(j)
        pair(j - 1)

    grad(jnp.int32(0))
    loop(4, grad_and_pair, 1)
    pair(jnp.int32(3))

    tok_wait(2)
    gains = gain[:, cols(y)]
    e0 = lengths[0, 0]
    e1 = e0 + lengths[0, 1]
    e2 = e1 + lengths[0, 2]

    def ids(pos):
        return (
            (pos >= e0).astype(jnp.int32) + (pos >= e1).astype(jnp.int32) + (pos >= e2).astype(jnp.int32)
        )

    def attend(i):
        r = pl.ds(pl.multiple_of(i * TOK, TOK), TOK)
        scores = nt(qh[r], kh[...]) * (HEAD**-0.5)
        qid = ids(lax.broadcasted_iota(jnp.int32, (TOK, GROUP), 0) + i * TOK)
        kid = ids(lax.broadcasted_iota(jnp.int32, (TOK, GROUP), 1))
        scores = jnp.where(qid == kid, scores, -1e30)
        expo = jnp.exp(scores - jnp.max(scores, axis=-1, keepdims=True))
        probs = (expo / jnp.sum(expo, axis=-1, keepdims=True)).astype(BF16)
        view[r] = rms(mm(probs, vh[...]), gains).astype(BF16)

    loop(4, attend)

    def rz_copy(to):
        return remote(zs.at[to], zr.at[z], rz_s.at[to], rz_r.at[z], wide_1=to)

    def fold(j):
        p = part_of(j)
        for e in range(1, NX):
            remote(xs.at[x, p], xr.at[e, p], rx_s.at[e, p], rx_r.at[e, p], wide_0=x).wait_recv()
        total = xs[x, p].astype(F32)
        for e in range(1, NX):
            total = total + xr[e, p].astype(F32)
        for t in range(4):
            zs[p * 4 + t] = total[:, t * 8 : (t + 1) * 8].astype(BF16)
        for t in range(4):

            @pl.when(p * 4 + t != z)
            def _():
                rz_copy(p * 4 + t).start()

    loop(4, fold)
    zr[z] = zs[z]
    gather_sent(wbuf, wz_s, wz_r, wx_s, wx_r, wc_s, wc_r)

    def summed(d, total):
        frm = lax.rem(z + NZ - d, NZ)
        remote(zs.at[frm], zr.at[frm], rz_s.at[frm], rz_r.at[frm], wide_1=frm).wait_recv()
        return total + zr[frm].astype(F32)

    total = lax.fori_loop(1, NZ, summed, zr[z].astype(F32))
    mbuf[0, c, 0] = (momentum_decay * mhalf[...] + total * TOKENS**-0.5).astype(BF16)
    gather(mbuf, mz_s, mz_r, mx_s, mx_r, mc_s, mc_r)

    def squares(i, sums):
        return tuple(
            s + jnp.sum(jnp.square(mbuf[i, 0, :, t].astype(F32)) + jnp.square(mbuf[i, 1, :, t].astype(F32)), axis=0)
            for t, s in enumerate(sums)
        )

    blank = jnp.zeros((8, HALF), F32)
    sums = lax.fori_loop(0, NX, squares, (blank, blank, blank))
    steps = tuple(
        step_size * lax.rsqrt(jnp.sum(jnp.sum(s, axis=1, keepdims=True), axis=0, keepdims=True) / HEAD**2 + epsilon)
        for s in sums
    )

    def moved_rows(w0, w1, m0, m1, step):
        v0 = w0 - m0 * step
        v1 = w1 - m1 * step
        before = jnp.sum(w0 * w0 + w1 * w1, axis=-1, keepdims=True) + epsilon
        after = jnp.sum(v0 * v0 + v1 * v1, axis=-1, keepdims=True) + epsilon
        ratio = jnp.sqrt(before) / jnp.sqrt(after)
        return v0 * ratio, v1 * ratio

    def renew(i):
        r = pl.ds(pl.multiple_of(i * TOK, TOK), TOK)
        for t in range(3):
            parts = moved_rows(*(tall(buf, i, h, t) for buf in (wbuf, mbuf) for h in range(2)), steps[t])
            for h in range(2):
                n2[t, r, h * HALF : (h + 1) * HALF] = parts[h].astype(BF16)

    loop(4, renew)
    for d in range(1, NY):
        tok_copy(2, d).wait_send()

    def turn(i):
        late = lax.div(i, 2)
        return (1 - late) * lax.rem(1 + 2 * i + 2 * c, 4) + late * (2 * i - 2)

    def o_copy(i):
        to = lax.rem(y + turn(i), NY)
        return remote(oblk.at[i], out.at[:, cols(y)], o_s.at[i], o_r.at[i], narrow=to)

    def apply(i):
        r = rows(lax.rem(y + turn(i), NY))
        qb = qh[r]
        pre_gate = mm(qb, n2[0])
        pre_up = mm(qb, n2[1])
        hidden = (pre_gate * jax.nn.sigmoid(pre_gate) * pre_up).astype(BF16)
        fast = rms(mm(hidden, n2[2]), gains).astype(BF16)
        oblk[i] = (view[r].astype(F32) + fast.astype(F32)).astype(BF16)

        @pl.when(i < NY - 1)
        def _():
            o_copy(i).start()

    loop(NY, apply)
    keep = pltpu.make_async_copy(oblk.at[NY - 1], out.at[:, cols(y)], o_own)
    keep.start()

    for t in range(3):
        m0, m1 = mbuf[0, 0, 0, t].astype(F32), mbuf[0, 1, 0, t].astype(F32)
        parts = moved_rows(wbuf[0, 0, 0, t].astype(F32), wbuf[0, 1, 0, t].astype(F32), m0, m1, steps[t])
        whole = jnp.concatenate(parts, axis=1)
        newv[t] = jnp.where(first, whole[:4], whole[4:]).astype(BF16)
        whole = jnp.concatenate([m0, m1], axis=1)
        momv[t] = jnp.where(first, whole[:4], whole[4:])
    done = [
        pltpu.make_async_copy(newv, new_out, small_sem.at[0]),
        pltpu.make_async_copy(momv, mom_out, small_sem.at[1]),
    ]
    for copy in done:
        copy.start()

    swap.wait_send()
    for t in range(2):
        for d in range(1, NY):
            tok_copy(t, d).wait_send()
    for b in range(NX):
        g_copy(b).wait_send()
    for j in range(4):
        for e in range(1, NX):
            rx_copy(jnp.int32(j), e).wait_send()

    def z_sent(d):
        rz_copy(lax.rem(z + d, NZ)).wait_send()

    loop(NZ, z_sent, 1)
    gather_sent(mbuf, mz_s, mz_r, mx_s, mx_r, mc_s, mc_r)
    for i in range(NY - 1):
        frm = lax.rem(y + NY - turn(i), NY)
        remote(oblk.at[i], out.at[:, cols(frm)], o_s.at[i], o_r.at[i], narrow=frm).wait()
    keep.wait()
    for copy in done:
        copy.wait()


def deliver(out_in, new_in, mom_in, out, ng, nu, nd, og, ou, od, outv, newv, momv, sems):
    quarter = TOK // 4
    parts = [pl.ds(i * quarter, quarter) for i in range(4)]
    get = [pltpu.make_async_copy(new_in, newv, sems.at[0]), pltpu.make_async_copy(mom_in, momv, sems.at[1])]
    get += [pltpu.make_async_copy(out_in.at[p], outv.at[p], sems.at[2 + i]) for i, p in enumerate(parts)]
    put = [
        [pltpu.make_async_copy(newv.at[t], o.at[0], sems.at[6 + t]) for t, o in enumerate((ng, nu, nd))],
        [pltpu.make_async_copy(momv.at[t], o.at[0], sems.at[9 + t]) for t, o in enumerate((og, ou, od))],
        *([pltpu.make_async_copy(outv.at[p], out.at[p], sems.at[12 + i])] for i, p in enumerate(parts)),
    ]
    for copy in get:
        copy.start()
    for copy, then in zip(get, put):
        copy.wait()
        for other in then:
            other.start()
    for then in put:
        for other in then:
            other.wait()


def per_device(queries, keys, values, view_lengths, gain, *weights):
    hbm = pl.BlockSpec(memory_space=pltpu.HBM)
    dma = pltpu.SemaphoreType.DMA
    sq = (HEAD, HEAD)
    row = (4, HEAD)
    gather_sems = [dma((NZ,)), dma((NZ,)), dma((NX, len(RUNS))), dma((NX, len(RUNS))), dma, dma]
    parts = pl.pallas_call(
        kernel,
        out_shape=(
            jax.ShapeDtypeStruct(queries.shape, BF16),
            jax.ShapeDtypeStruct((3, *row), BF16),
            jax.ShapeDtypeStruct((3, *row), F32),
        ),
        in_specs=[hbm] * 11,
        out_specs=(hbm,) * 3,
        scratch_shapes=[
            pltpu.SMEM(view_lengths.shape, jnp.int32),
            pltpu.VMEM((1, gain.shape[0]), F32),
            pltpu.VMEM((3, *row), BF16),
            pltpu.VMEM((3, *row), BF16),
            pltpu.VMEM((3, *row), F32),
            dma((8,)),
            *[pltpu.VMEM(sq, BF16)] * 8,
            pltpu.VMEM((6, *row), F32),
            pltpu.VMEM((6, *row), F32),
            pltpu.VMEM((3, 8, HALF), F32),
            pltpu.VMEM((NX, 2, NZ, 3, 8, HALF), BF16),
            pltpu.VMEM((3, HEAD, HEAD), BF16),
            pltpu.VMEM((4, NX, 3, 32, HALF), F32),
            pltpu.VMEM((4, NX, 3, 32, HALF), BF16),
            pltpu.VMEM((4, NX, 3, 32, HALF), BF16),
            pltpu.VMEM((NX, 4, 3, 32, HALF), BF16),
            pltpu.VMEM((NX, 4, 3, 32, HALF), BF16),
            pltpu.VMEM((NZ, 3, 8, HALF), BF16),
            pltpu.VMEM((NZ, 3, 8, HALF), BF16),
            pltpu.VMEM((NX, 2, NZ, 3, 8, HALF), BF16),
            pltpu.VMEM((3, HEAD, HEAD), BF16),
            pltpu.VMEM(sq, BF16),
            pltpu.VMEM((NY, TOK, HEAD), BF16),
            dma((3, NY)), dma((3, NY)), dma((3,)), dma((2,)),
            *gather_sems,
            *gather_sems,
            dma((NX,)), dma((NX,)), dma((NX, 4)), dma((NX, 4)), dma((NZ,)), dma((NZ,)),
            dma((NY,)), dma((NY,)), dma,
        ],
        compiler_params=pltpu.CompilerParams(
            collective_id=0, has_side_effects=True, vmem_limit_bytes=67_043_328
        ),
    )(queries, keys, values, view_lengths, gain.reshape(1, -1), *weights)
    return pl.pallas_call(
        deliver,
        out_shape=(
            jax.ShapeDtypeStruct(queries.shape, BF16),
            *[jax.ShapeDtypeStruct((1, *row), BF16)] * 3,
            *[jax.ShapeDtypeStruct((1, *row), F32)] * 3,
        ),
        in_specs=[hbm] * 3,
        out_specs=(hbm,) * 7,
        scratch_shapes=[
            pltpu.VMEM(queries.shape, BF16),
            pltpu.VMEM((3, *row), BF16),
            pltpu.VMEM((3, *row), F32),
            dma((16,)),
        ],
        compiler_params=pltpu.CompilerParams(vmem_limit_bytes=67_043_328),
    )(*parts)


def solution(mesh):
    split = Mesh(
        mesh.devices.reshape(NX, NZ, 2, mesh.shape["narrow"]),
        ("wide_0", "wide_1", "wide_2", "narrow"),
    )
    rows = P("narrow", WIDE, None)
    return jax.shard_map(
        per_device,
        mesh=split,
        in_specs=(*[P(WIDE_NARROW, None)] * 3, P(WIDE, None), P(), *[rows] * 6),
        out_specs=(P(WIDE_NARROW, None), *[rows] * 6),
        check_vma=False,
    )
```

```python
import functools

import jax
import jax.numpy as jnp
from jax import lax
from jax.experimental import pallas as pl
from jax.experimental.pallas import tpu as pltpu
from jax.sharding import Mesh
from jax.sharding import PartitionSpec as P

WIDE = ("wide_0", "wide_1", "wide_2")
WIDE_NARROW = ("wide_0", "wide_1", "wide_2", "narrow")
MESH = pl.DeviceIdType.MESH

momentum_decay = 0.9
step_size = 0.02
epsilon = 1e-06

NX, NZ, NY = 4, 16, 4
NEAR = 3
STAGES = tuple(range(NEAR, NZ // 2, NEAR))
LAST = STAGES[-1] + 1
RUNS = (
    (0, 1),
    *((a, NEAR) for p in STAGES for a in (p - NEAR + 1, NZ - p)),
    (LAST, NZ + 1 - 2 * LAST),
)
HEAD = 512
HALF = 256
GROUP = 512
TOK = 128
TOKENS = 65536
F32 = jnp.float32
BF16 = jnp.bfloat16


def nt(a, b):
    return lax.dot_general(a, b, (((1,), (1,)), ((), ())), preferred_element_type=F32)


def mm(a, b):
    return jnp.dot(a, b, preferred_element_type=F32)


def rms(field, gains):
    return field * lax.rsqrt(jnp.mean(field * field, axis=-1, keepdims=True) + epsilon) * gains


def remote(src, dst, send, recv, **where):
    return pltpu.make_async_remote_copy(
        src_ref=src, dst_ref=dst, send_sem=send, recv_sem=recv, device_id=where, device_id_type=MESH
    )


def loop(n, body, start=0):
    def step(i, carry):
        body(i)
        return carry

    lax.fori_loop(start, n, step, 0)


def kernel(
    q_in, k_in, v_in, lengths_in, gain_in, wg, wu, wd, mg, mu, md,
    out, new_out, mom_out,
    lengths, gain, wrow, newv, momv, small_sem,
    qh, kh, vh, kt, ht, hid, dg, du, ex, exr, mhalf, wbuf, w2, own, gsend, grecv,
    xs, xr, zs, zr, mbuf, n2, view, oblk,
    tok_send, tok_recv, tok_own, ex_sem, wz_s, wz_r, wx_s, wx_r, wc_s, wc_r,
    mz_s, mz_r, mx_s, mx_r, mc_s, mc_r, gs_s, gs_r, rx_s, rx_r, rz_s, rz_r, o_s, o_r, o_own,
):
    x = lax.axis_index("wide_0")
    z = lax.axis_index("wide_1")
    c = lax.axis_index("wide_2")
    y = lax.axis_index("narrow")
    other = 1 - c
    side = 1 + 2 * c

    small = [pltpu.make_async_copy(w.at[0], wrow.at[t], small_sem.at[t]) for t, w in enumerate((wg, wu, wd))]
    small += [pltpu.make_async_copy(m.at[0], ex.at[3 + t], small_sem.at[3 + t]) for t, m in enumerate((mg, mu, md))]
    small += [
        pltpu.make_async_copy(lengths_in, lengths, small_sem.at[6]),
        pltpu.make_async_copy(gain_in, gain, small_sem.at[7]),
    ]
    for copy in small:
        copy.start()

    barrier = pltpu.get_barrier_semaphore()
    pl.semaphore_signal(barrier, inc=1, device_id={"wide_2": other}, device_id_type=MESH)
    for d in range(1, NY):
        pl.semaphore_signal(
            barrier, inc=1, device_id={"narrow": lax.rem(y + d, NY)}, device_id_type=MESH
        )
    for d in range(1, NX):
        pl.semaphore_signal(
            barrier, inc=1, device_id={"wide_0": lax.rem(x + d, NX)}, device_id_type=MESH
        )

    def greet(d):
        pl.semaphore_signal(
            barrier, inc=1, device_id={"wide_1": lax.rem(z + d, NZ)}, device_id_type=MESH
        )

    for d in range(1, NEAR + 1):
        greet(d)
        greet(NZ - d)
    for copy in small:
        copy.wait()
    ex[:3] = wrow[...].astype(F32)
    pl.semaphore_wait(barrier, NY - 1 + NX - 1 + 2 * NEAR + 1)

    def cols(who):
        return pl.ds(pl.multiple_of(who * HEAD, HEAD), HEAD)

    def rows(who):
        return pl.ds(pl.multiple_of(who * TOK, TOK), TOK)

    trio = ((k_in, kh), (v_in, vh), (q_in, qh))

    def tok_copy(t, d):
        src, dst = trio[t]
        to = lax.rem(y + d, NY)
        return remote(
            src.at[:, cols(to)], dst.at[rows(y)], tok_send.at[t, d], tok_recv.at[t, d], narrow=to
        )

    def tok_wait(t):
        src, dst = trio[t]
        for d in range(1, NY):
            frm = lax.rem(y + NY - d, NY)
            remote(
                src.at[:, cols(y)], dst.at[rows(frm)], tok_send.at[t, d], tok_recv.at[t, d], narrow=frm
            ).wait_recv()
        tok_local(t).wait()

    def tok_local(t):
        src, dst = trio[t]
        return pltpu.make_async_copy(src.at[:, cols(y)], dst.at[rows(y)], tok_own.at[t])

    swap = remote(ex, exr, ex_sem.at[0], ex_sem.at[1], wide_2=other)
    swap.start()
    for t in range(3):
        for d in (side, 4 - side, 2):
            tok_copy(t, d).start()
        tok_local(t).start()

    def z_copy(buf, z_s, z_r, via, hop):
        d = (via + hop) % NZ
        return remote(
            buf.at[0, c, via], buf.at[0, c, d], z_s.at[d], z_r.at[d], wide_1=lax.rem(z + hop, NZ)
        )

    def x_copy(buf, x_s, x_r, e, k):
        a, n = RUNS[k]
        return remote(
            buf.at[0, c, pl.ds(a, n)], buf.at[e, c, pl.ds(a, n)], x_s.at[e, k], x_r.at[e, k],
            wide_0=lax.rem(x + e, NX),
        )

    def gather(buf, z_s, z_r, x_s, x_r, c_s, c_r, meanwhile=None):
        def across(e, k):
            a, n = RUNS[k]
            part = buf.at[e, c, pl.ds(a, n)]
            remote(part, part, c_s, c_r, wide_2=other).start()

        def forward(k, late=False):
            for e in (2, side, 4 - side) if late else (side, 4 - side, 2):
                x_copy(buf, x_s, x_r, e, k).start()
            across(0, k)

        def landed(d):
            z_copy(buf, z_s, z_r, d, 0).wait_recv()

        def arrived(k):
            for e in (1, 3, 2):
                x_copy(buf, x_s, x_r, e, k).wait_recv()
                across(e, k)

        def onward(p):
            hops = range(min(NEAR, NZ // 2 - p), 0, -1)
            for hop in hops:
                z_copy(buf, z_s, z_r, p, hop).start()

        def backward(p):
            for hop in range(min(NEAR, NZ // 2 - 1 - p), 0, -1):
                z_copy(buf, z_s, z_r, (NZ - p) % NZ, NZ - hop).start()

        onward(0)
        backward(0)
        forward(0)
        for k, p in enumerate(STAGES):
            landed(p)
            onward(p)
            landed(NZ - p)
            backward(p)
            for d in range(p - NEAR + 1, p):
                landed(d)
            forward(2 * k + 1)
            for d in range(NZ - p + 1, NZ - p + NEAR):
                landed(d)
            forward(2 * k + 2)
            if k == 0:
                arrived(0)
        for d in range(LAST, NZ + 1 - LAST):
            landed(d)
        forward(len(RUNS) - 1, True)
        if meanwhile is not None:
            meanwhile()
        for k in range(1, len(RUNS)):
            arrived(k)
        part = buf.at[:, other]
        remote(part, part, c_s, c_r, wide_2=other).wait_recv()

    def gather_sent(buf, z_s, z_r, x_s, x_r, c_s, c_r):
        for d in range(1, NZ):
            z_copy(buf, z_s, z_r, 0, d).wait_send()
        for k in range(len(RUNS)):
            for e in range(1, NX):
                x_copy(buf, x_s, x_r, e, k).wait_send()
        part = buf.at[:, c]
        remote(part, part, c_s, c_r, wide_2=other).wait_send()

    def tall(buf, i, h, t):
        e = lax.rem(x + NX - i, NX)
        return jnp.concatenate(
            [buf[e, h, lax.rem(z + NZ - b, NZ), t].astype(F32) for b in range(NZ)], axis=0
        )

    swap.wait_recv()
    mine, theirs = ex[...], exr[...]
    first = c == 0
    rows8 = jnp.concatenate(
        [jnp.where(first, mine, theirs), jnp.where(first, theirs, mine)], axis=1
    )
    half = jnp.where(first, rows8[:, :, :HALF], rows8[:, :, HALF:])
    wbuf[0, c, 0] = half[:3].astype(BF16)
    mhalf[...] = half[3:]

    def turn_keys():
        tok_wait(0)
        kt[...] = kh[...].T

    gather(wbuf, wz_s, wz_r, wx_s, wx_r, wc_s, wc_r, turn_keys)

    def square(i):
        r = pl.ds(pl.multiple_of(i * TOK, TOK), TOK)
        for t in range(3):
            for h in range(2):
                w2[t, r, h * HALF : (h + 1) * HALF] = tall(wbuf, i, h, t).astype(BF16)

    loop(4, square)
    tok_wait(1)


    def back(i):
        r = pl.ds(pl.multiple_of(i * TOK, TOK), TOK)
        kb = kh[r]
        pre_gate = mm(kb, w2[0])
        pre_up = mm(kb, w2[1])
        d_hidden = -nt(vh[r], w2[2])
        sig = jax.nn.sigmoid(pre_gate)
        activ = pre_gate * sig
        hid[r] = (activ * pre_up).astype(BF16)
        dg[r] = (d_hidden * pre_up * (sig * (1.0 + pre_gate * (1.0 - sig)))).astype(BF16)
        du[r] = (d_hidden * activ).astype(BF16)

    loop(4, back)
    ht[...] = hid[...].T

    def g_copy(b):
        return remote(gsend.at[b], grecv.at[b], gs_s.at[b], gs_r.at[b], wide_2=other)

    def part_of(j):
        return lax.rem(lax.div(z, 4) + 2 + j + lax.div(j * (j - 1), 2), 4)

    def grad(j):
        p = part_of(j)
        quarter = [pl.ds(pl.multiple_of(b * TOK + p * 32, 32), 32) for b in range(NX)]
        kb = jnp.concatenate([kt[r] for r in quarter], axis=0)
        hb = jnp.concatenate([ht[r] for r in quarter], axis=0)
        for t, g in enumerate((mm(kb, dg[...]), mm(kb, du[...]), -mm(hb, vh[...]))):
            keep = jnp.where(first, g[:, :HALF], g[:, HALF:])
            give = jnp.where(first, g[:, HALF:], g[:, :HALF]).astype(BF16)
            for b in range(NX):
                own[p, b, t] = keep[b * 32 : (b + 1) * 32]
                gsend[p, b, t] = give[b * 32 : (b + 1) * 32]
        g_copy(p).start()

    def rx_copy(j, e):
        to = lax.rem(x + e, NX)
        p = part_of(j)
        return remote(xs.at[to, p], xr.at[e, p], rx_s.at[e, p], rx_r.at[e, p], wide_0=to)

    def pair(j):
        p = part_of(j)
        g_copy(p).wait_recv()
        for b in range(NX):
            for t in range(3):
                xs[b, p, t] = (own[p, b, t] + grecv[p, b, t].astype(F32)).astype(BF16)
        for e in (side, 4 - side, 2):
            rx_copy(j, e).start()

    def grad_and_pair(j):
        grad(j)
        pair(j - 1)

    grad(jnp.int32(0))
    loop(4, grad_and_pair, 1)
    pair(jnp.int32(3))

    tok_wait(2)
    gains = gain[:, cols(y)]
    e0 = lengths[0, 0]
    e1 = e0 + lengths[0, 1]
    e2 = e1 + lengths[0, 2]

    def ids(pos):
        return (
            (pos >= e0).astype(jnp.int32) + (pos >= e1).astype(jnp.int32) + (pos >= e2).astype(jnp.int32)
        )

    def attend(i):
        r = pl.ds(pl.multiple_of(i * TOK, TOK), TOK)
        scores = nt(qh[r], kh[...]) * (HEAD**-0.5)
        qid = ids(lax.broadcasted_iota(jnp.int32, (TOK, GROUP), 0) + i * TOK)
        kid = ids(lax.broadcasted_iota(jnp.int32, (TOK, GROUP), 1))
        scores = jnp.where(qid == kid, scores, -1e30)
        expo = jnp.exp(scores - jnp.max(scores, axis=-1, keepdims=True))
        probs = (expo / jnp.sum(expo, axis=-1, keepdims=True)).astype(BF16)
        view[r] = rms(mm(probs, vh[...]), gains).astype(BF16)

    loop(4, attend)

    def rz_copy(to):
        return remote(zs.at[to], zr.at[z], rz_s.at[to], rz_r.at[z], wide_1=to)

    def fold(j):
        p = part_of(j)
        for e in range(1, NX):
            remote(xs.at[x, p], xr.at[e, p], rx_s.at[e, p], rx_r.at[e, p], wide_0=x).wait_recv()
        total = xs[x, p].astype(F32)
        for e in range(1, NX):
            total = total + xr[e, p].astype(F32)
        for t in range(4):
            zs[p * 4 + t] = total[:, t * 8 : (t + 1) * 8].astype(BF16)
        for t in range(4):

            @pl.when(p * 4 + t != z)
            def _():
                rz_copy(p * 4 + t).start()

    loop(4, fold)
    zr[z] = zs[z]

    def summed(d, total):
        frm = lax.rem(z + NZ - d, NZ)
        remote(zs.at[frm], zr.at[frm], rz_s.at[frm], rz_r.at[frm], wide_1=frm).wait_recv()
        return total + zr[frm].astype(F32)

    total = lax.fori_loop(1, NZ, summed, zr[z].astype(F32))
    mbuf[0, c, 0] = (momentum_decay * mhalf[...] + total * TOKENS**-0.5).astype(BF16)
    gather(mbuf, mz_s, mz_r, mx_s, mx_r, mc_s, mc_r)

    def squares(i, sums):
        return tuple(
            s + jnp.sum(jnp.square(mbuf[i, 0, :, t].astype(F32)) + jnp.square(mbuf[i, 1, :, t].astype(F32)), axis=0)
            for t, s in enumerate(sums)
        )

    blank = jnp.zeros((8, HALF), F32)
    sums = lax.fori_loop(0, NX, squares, (blank, blank, blank))
    steps = tuple(
        step_size * lax.rsqrt(jnp.sum(jnp.sum(s, axis=1, keepdims=True), axis=0, keepdims=True) / HEAD**2 + epsilon)
        for s in sums
    )

    def moved_rows(w0, w1, m0, m1, step):
        v0 = w0 - m0 * step
        v1 = w1 - m1 * step
        before = jnp.sum(w0 * w0 + w1 * w1, axis=-1, keepdims=True) + epsilon
        after = jnp.sum(v0 * v0 + v1 * v1, axis=-1, keepdims=True) + epsilon
        ratio = jnp.sqrt(before) / jnp.sqrt(after)
        return v0 * ratio, v1 * ratio

    def renew(i):
        r = pl.ds(pl.multiple_of(i * TOK, TOK), TOK)
        for t in range(3):
            parts = moved_rows(*(tall(buf, i, h, t) for buf in (wbuf, mbuf) for h in range(2)), steps[t])
            for h in range(2):
                n2[t, r, h * HALF : (h + 1) * HALF] = parts[h].astype(BF16)

    loop(4, renew)

    def turn(i):
        late = lax.div(i, 2)
        return (1 - late) * lax.rem(1 + 2 * i + 2 * c, 4) + late * (2 * i - 2)

    def o_copy(i):
        to = lax.rem(y + turn(i), NY)
        return remote(oblk.at[i], out.at[:, cols(y)], o_s.at[i], o_r.at[i], narrow=to)

    def apply(i):
        r = rows(lax.rem(y + turn(i), NY))
        qb = qh[r]
        pre_gate = mm(qb, n2[0])
        pre_up = mm(qb, n2[1])
        hidden = (pre_gate * jax.nn.sigmoid(pre_gate) * pre_up).astype(BF16)
        fast = rms(mm(hidden, n2[2]), gains).astype(BF16)
        oblk[i] = (view[r].astype(F32) + fast.astype(F32)).astype(BF16)

        @pl.when(i < NY - 1)
        def _():
            o_copy(i).start()

    loop(NY, apply)
    keep = pltpu.make_async_copy(oblk.at[NY - 1], out.at[:, cols(y)], o_own)
    keep.start()

    for t in range(3):
        m0, m1 = mbuf[0, 0, 0, t].astype(F32), mbuf[0, 1, 0, t].astype(F32)
        parts = moved_rows(wbuf[0, 0, 0, t].astype(F32), wbuf[0, 1, 0, t].astype(F32), m0, m1, steps[t])
        whole = jnp.concatenate(parts, axis=1)
        newv[t] = jnp.where(first, whole[:4], whole[4:]).astype(BF16)
        whole = jnp.concatenate([m0, m1], axis=1)
        momv[t] = jnp.where(first, whole[:4], whole[4:])
    done = [
        pltpu.make_async_copy(newv, new_out, small_sem.at[0]),
        pltpu.make_async_copy(momv, mom_out, small_sem.at[1]),
    ]
    for copy in done:
        copy.start()

    swap.wait_send()
    for t in range(3):
        for d in range(1, NY):
            tok_copy(t, d).wait_send()
    for b in range(NX):
        g_copy(b).wait_send()
    for j in range(4):
        for e in range(1, NX):
            rx_copy(jnp.int32(j), e).wait_send()

    def z_sent(d):
        rz_copy(lax.rem(z + d, NZ)).wait_send()

    loop(NZ, z_sent, 1)
    gather_sent(wbuf, wz_s, wz_r, wx_s, wx_r, wc_s, wc_r)
    gather_sent(mbuf, mz_s, mz_r, mx_s, mx_r, mc_s, mc_r)
    for i in range(NY - 1):
        frm = lax.rem(y + NY - turn(i), NY)
        remote(oblk.at[i], out.at[:, cols(frm)], o_s.at[i], o_r.at[i], narrow=frm).wait()
    keep.wait()
    for copy in done:
        copy.wait()


def deliver(out_in, new_in, mom_in, out, ng, nu, nd, og, ou, od, outv, newv, momv, sems):
    quarter = TOK // 4
    parts = [pl.ds(i * quarter, quarter) for i in range(4)]
    get = [pltpu.make_async_copy(new_in, newv, sems.at[0]), pltpu.make_async_copy(mom_in, momv, sems.at[1])]
    get += [pltpu.make_async_copy(out_in.at[p], outv.at[p], sems.at[2 + i]) for i, p in enumerate(parts)]
    put = [
        [pltpu.make_async_copy(newv.at[t], o.at[0], sems.at[6 + t]) for t, o in enumerate((ng, nu, nd))],
        [pltpu.make_async_copy(momv.at[t], o.at[0], sems.at[9 + t]) for t, o in enumerate((og, ou, od))],
        *([pltpu.make_async_copy(outv.at[p], out.at[p], sems.at[12 + i])] for i, p in enumerate(parts)),
    ]
    for copy in get:
        copy.start()
    for copy, then in zip(get, put):
        copy.wait()
        for other in then:
            other.start()
    for then in put:
        for other in then:
            other.wait()


def per_device(queries, keys, values, view_lengths, gain, *weights):
    hbm = pl.BlockSpec(memory_space=pltpu.HBM)
    dma = pltpu.SemaphoreType.DMA
    sq = (HEAD, HEAD)
    row = (4, HEAD)
    gather_sems = [dma((NZ,)), dma((NZ,)), dma((NX, len(RUNS))), dma((NX, len(RUNS))), dma, dma]
    parts = pl.pallas_call(
        kernel,
        out_shape=(
            jax.ShapeDtypeStruct(queries.shape, BF16),
            jax.ShapeDtypeStruct((3, *row), BF16),
            jax.ShapeDtypeStruct((3, *row), F32),
        ),
        in_specs=[hbm] * 11,
        out_specs=(hbm,) * 3,
        scratch_shapes=[
            pltpu.SMEM(view_lengths.shape, jnp.int32),
            pltpu.VMEM((1, gain.shape[0]), F32),
            pltpu.VMEM((3, *row), BF16),
            pltpu.VMEM((3, *row), BF16),
            pltpu.VMEM((3, *row), F32),
            dma((8,)),
            *[pltpu.VMEM(sq, BF16)] * 8,
            pltpu.VMEM((6, *row), F32),
            pltpu.VMEM((6, *row), F32),
            pltpu.VMEM((3, 8, HALF), F32),
            pltpu.VMEM((NX, 2, NZ, 3, 8, HALF), BF16),
            pltpu.VMEM((3, HEAD, HEAD), BF16),
            pltpu.VMEM((4, NX, 3, 32, HALF), F32),
            pltpu.VMEM((4, NX, 3, 32, HALF), BF16),
            pltpu.VMEM((4, NX, 3, 32, HALF), BF16),
            pltpu.VMEM((NX, 4, 3, 32, HALF), BF16),
            pltpu.VMEM((NX, 4, 3, 32, HALF), BF16),
            pltpu.VMEM((NZ, 3, 8, HALF), BF16),
            pltpu.VMEM((NZ, 3, 8, HALF), BF16),
            pltpu.VMEM((NX, 2, NZ, 3, 8, HALF), BF16),
            pltpu.VMEM((3, HEAD, HEAD), BF16),
            pltpu.VMEM(sq, BF16),
            pltpu.VMEM((NY, TOK, HEAD), BF16),
            dma((3, NY)), dma((3, NY)), dma((3,)), dma((2,)),
            *gather_sems,
            *gather_sems,
            dma((NX,)), dma((NX,)), dma((NX, 4)), dma((NX, 4)), dma((NZ,)), dma((NZ,)),
            dma((NY,)), dma((NY,)), dma,
        ],
        compiler_params=pltpu.CompilerParams(
            collective_id=0, has_side_effects=True, vmem_limit_bytes=67_043_328
        ),
    )(queries, keys, values, view_lengths, gain.reshape(1, -1), *weights)
    return pl.pallas_call(
        deliver,
        out_shape=(
            jax.ShapeDtypeStruct(queries.shape, BF16),
            *[jax.ShapeDtypeStruct((1, *row), BF16)] * 3,
            *[jax.ShapeDtypeStruct((1, *row), F32)] * 3,
        ),
        in_specs=[hbm] * 3,
        out_specs=(hbm,) * 7,
        scratch_shapes=[
            pltpu.VMEM(queries.shape, BF16),
            pltpu.VMEM((3, *row), BF16),
            pltpu.VMEM((3, *row), F32),
            dma((16,)),
        ],
        compiler_params=pltpu.CompilerParams(vmem_limit_bytes=67_043_328),
    )(*parts)


def solution(mesh):
    split = Mesh(
        mesh.devices.reshape(NX, NZ, 2, mesh.shape["narrow"]),
        ("wide_0", "wide_1", "wide_2", "narrow"),
    )
    rows = P("narrow", WIDE, None)
    return jax.shard_map(
        per_device,
        mesh=split,
        in_specs=(*[P(WIDE_NARROW, None)] * 3, P(WIDE, None), P(), *[rows] * 6),
        out_specs=(P(WIDE_NARROW, None), *[rows] * 6),
        check_vma=False,
    )
```
